32 devices in a mesh: rep: 4 (over z), gy: 2 (over y), gz: 4 (over x, core).
Axes of the slice: x: 2, y: 2, z: 4, core: 2. Of those that a mesh axis runs over, the one named last changes fastest.
Arguments:
- charges: float32 [1024, 256, 128], P(('rep', 'gz'), 'gy'), may hold values from -6 to 6
- green: float32 [256, 256, 128], P('rep', ('gy', 'gz')), may hold values from 0.1 to 3
Outputs:
- potential: float32 [1024, 256, 128], P(('rep', 'gz'), 'gy')
The draws below stay inside these ranges and needn't reach their ends.
All inputs are finite; a program needn't handle non-finite values.
Results may differ from the reference program's by a relative error of at most 0.00007.
Values sent between devices are 32-bit elements; how exact they have to be, the bound alone decides.
A program may use at most 64 MiB of HBM per device.

```python
import math
import jax
import jax.numpy as jnp
from jax import lax

NG = 256
NZ = 128
REPLICAS = 4


def levels(key, dims, shards, low, top_value):
    gain = 1.0
    for axis_at, blocks in shards:
        steps = jax.random.uniform(jax.random.fold_in(jax.random.fold_in(key, 6), axis_at), (blocks,), jnp.float32, low / len(shards), top_value / len(shards))
        gain = gain * jnp.repeat(jnp.exp(steps), dims[axis_at] // blocks).reshape((-1,) + (1,) * (len(dims) - 1 - axis_at))
    return gain


def bell_draw(stream_key, shape, scale, reach, split=(), kind=jnp.bfloat16):
    array = scale * jax.random.normal(stream_key, shape, jnp.float32)
    if split:
        array = array * levels(stream_key, shape, split, -0.22, 0.18)
    return jnp.clip(array, -reach, reach).astype(kind)


def setup_inputs(seed: int = 0) -> dict:
    streams_of = jax.random.split(jax.random.key(seed), 3)
    return {
        "charges": bell_draw(streams_of[0], (REPLICAS * NG, NG, NZ), 1.0, 6.0, ((0, 16), (1, 2)), jnp.float32),
        "green": jnp.clip(jnp.exp(math.log(3.0) - 3.4011974 * jax.random.uniform(streams_of[1], (NG, NG, NZ), jnp.float32) ** levels(streams_of[1], (NG, NG, NZ), ((0, 4), (1, 8)), -0.2, 0.2)), 0.1, 3.0),
    }


def reference(charges, green):
    stacked = charges.reshape(REPLICAS, NG, NG, NZ)

    def single(charge):
        spectrum = jnp.fft.fftn(charge) * green
        return jnp.real(jnp.fft.ifftn(spectrum)).astype(jnp.float32)

    return lax.map(single, stacked).reshape(REPLICAS * NG, NG, NZ)
```

```python
import functools
import math

import jax
import jax.numpy as jnp
import numpy as np
from jax import lax
from jax.experimental import pallas as pl
from jax.experimental.pallas import tpu as pltpu
from jax.sharding import PartitionSpec as P

NG = 256
NZ = 128


two_pi = 2.0 * math.pi
highest = lax.Precision.HIGHEST


def tables(length, rows_index, cols_index):
    phase = rows_index[:, None] * cols_index[None, :] % length
    angle = phase.astype(jnp.float32) * (two_pi / length)
    return (jnp.cos(angle), jnp.sin(angle))


def reflect(values):
    return jnp.roll(jnp.flip(values, (1, 2)), (1, 1), axis=(1, 2))


def slab_plan(charges, green):
    gy_count = lax.axis_size("gy")
    gz_count = lax.axis_size("gz")
    groups = gy_count * gz_count
    half = NZ // 2
    per_device = half // groups
    col_block = charges.shape[1]
    depth = jnp.arange(NZ, dtype=jnp.int32)
    bins = jnp.arange(half, dtype=jnp.int32)
    indices = jnp.arange(NG, dtype=jnp.int32)
    cos_depth, sin_depth = tables(NZ, depth, bins)
    alternate = (1 - 2 * (depth % 2)).astype(jnp.float32)
    sin_packed = jnp.where(bins[None, :] == 0, -alternate[:, None], sin_depth)
    spec_re = jnp.einsum("xyz,zk->kxy", charges, cos_depth, precision=highest)
    spec_im = -jnp.einsum("xyz,zk->kxy", charges, sin_packed, precision=highest)
    own = jnp.moveaxis(green[:, :, :half], 2, 0)
    mirror = jnp.concatenate(
        [green[:, :, half : half + 1], jnp.flip(green[:, :, half + 1 :], 2)], axis=2
    )
    mirror = jnp.moveaxis(mirror, 2, 0)
    own, mirror = (
        lax.all_to_all(own, ("gy", "gz"), split_axis=0, concat_axis=2, tiled=True),
        lax.all_to_all(mirror, ("gy", "gz"), split_axis=0, concat_axis=2, tiled=True),
    )
    own, mirror = (
        lax.all_gather(own, "rep", axis=1, tiled=True),
        lax.all_gather(mirror, "rep", axis=1, tiled=True),
    )
    plane_re, plane_im = (
        lax.all_to_all(spec_re, ("gy", "gz"), split_axis=0, concat_axis=1, tiled=True),
        lax.all_to_all(spec_im, ("gy", "gz"), split_axis=0, concat_axis=1, tiled=True),
    )
    plane_re = plane_re.reshape(per_device, gy_count, NG, col_block)
    plane_im = plane_im.reshape(per_device, gy_count, NG, col_block)
    cos_plain, sin_plain = tables(NG, indices, indices)
    wide_cos = cos_plain.reshape(NG, gy_count, col_block)
    wide_sin = sin_plain.reshape(NG, gy_count, col_block)

    def second_in(matrix, values):
        return jnp.einsum("kgc,bgxc->bxk", matrix, values, precision=highest)

    def first_in(matrix, values):
        return jnp.einsum("kx,bxj->bkj", matrix, values, precision=highest)

    inner_re = second_in(wide_cos, plane_re) + second_in(wide_sin, plane_im)
    inner_im = second_in(wide_cos, plane_im) - second_in(wide_sin, plane_re)
    freq_re = first_in(cos_plain, inner_re) + first_in(sin_plain, inner_im)
    freq_im = first_in(cos_plain, inner_im) - first_in(sin_plain, inner_re)
    slot = lax.axis_index("gy") * gz_count + lax.axis_index("gz")
    packed = ((slot == 0) & (jnp.arange(per_device) == 0))[:, None, None]
    plain_gain = 0.5 * (own + reflect(mirror))
    first_gain = jnp.where(packed, 0.5 * (own + reflect(own)), plain_gain)
    second_gain = jnp.where(packed, 0.5 * (mirror + reflect(mirror)), plain_gain)
    mean_gain = 0.5 * (first_gain + second_gain)
    odd_gain = 0.5 * (first_gain - second_gain)
    prod_re = freq_re * mean_gain + reflect(freq_re) * odd_gain
    prod_im = freq_im * mean_gain - reflect(freq_im) * odd_gain
    undo_re = first_in(cos_plain, prod_re) - first_in(sin_plain, prod_im)
    undo_im = first_in(sin_plain, prod_re) + first_in(cos_plain, prod_im)

    def second_out(matrix, values):
        return jnp.einsum("kgc,bxk->bgxc", matrix, values, precision=highest)

    cells_re = second_out(wide_cos, undo_re) - second_out(wide_sin, undo_im)
    cells_im = second_out(wide_sin, undo_re) + second_out(wide_cos, undo_im)
    cells_re = cells_re.reshape(per_device, gy_count * NG, col_block)
    cells_im = cells_im.reshape(per_device, gy_count * NG, col_block)
    home_re, home_im = (
        lax.all_to_all(cells_re, ("gy", "gz"), split_axis=1, concat_axis=0, tiled=True),
        lax.all_to_all(cells_im, ("gy", "gz"), split_axis=1, concat_axis=0, tiled=True),
    )
    weight = jnp.where(bins == 0, 1.0, 2.0).astype(jnp.float32)
    cos_back = (cos_depth * weight[None, :]).T
    sin_back = jnp.where(bins[:, None] == 0, alternate[None, :], -2.0 * sin_depth.T)
    result_field = jnp.einsum("kxy,kz->xyz", home_re, cos_back, precision=highest)
    result_field = result_field + jnp.einsum("kxy,kz->xyz", home_im, sin_back, precision=highest)
    return result_field / (NG * NG * NZ)


f32 = jnp.float32
bf16 = jnp.bfloat16
MESH = pl.DeviceIdType.MESH
PARTS = 2
HALVES = 2


def split(values):
    high = values.astype(bf16)
    return high, (values - high.astype(f32)).astype(bf16)


def stacked_table(table, axis):
    rounded = table.astype(jnp.bfloat16)
    return jnp.asarray(np.stack([rounded, (table - rounded.astype(np.float64)).astype(jnp.bfloat16)], axis=axis))


def dot(left, right, dims=((1,), (0,))):
    return lax.dot_general(left, right, (dims, ((), ())), preferred_element_type=f32)


def dot_table(values, table_high, table_low, dims=((1,), (0,))):
    high, low = split(values)
    return dot(high, table_high, dims) + (dot(low, table_high, dims) + dot(high, table_low, dims))


def table_dot(table_high, table_low, values, dims=((1,), (0,))):
    high, low = split(values)
    return dot(table_high, high, dims) + (dot(table_high, low, dims) + dot(table_low, high, dims))


def depth_tables(length, groups, bins_each):
    per_part = bins_each // PARTS
    forward, back = [], []
    z = np.arange(length)
    alternate = 1.0 - 2.0 * (z % 2)
    for start in range(0, groups * bins_each, per_part):
        for imaginary in (False, True):
            for k in range(start, start + per_part):
                angle = 2.0 * np.pi * ((k * z) % length) / length
                if k == 0:
                    forward.append(alternate if imaginary else np.ones(length))
                    back.append(alternate if imaginary else np.ones(length))
                else:
                    forward.append(-np.sin(angle) if imaginary else np.cos(angle))
                    back.append(-2.0 * np.sin(angle) if imaginary else 2.0 * np.cos(angle))
    return np.stack(forward), np.stack(back)


def wide_table(table, axis):
    rounded = table.astype(jnp.bfloat16)
    low = (table - rounded.astype(np.float64)).astype(jnp.bfloat16)
    both = np.concatenate([rounded, rounded], axis=1 - axis)
    return jnp.asarray(np.concatenate([both, np.concatenate([low, np.zeros_like(low)], axis=1 - axis)], axis=axis))


def depth_in(table, cells, out):
    groups, parts, _, cols = out.shape
    rows, depth, step = cells.shape[0], cells.shape[2], 8

    def body(i, carry):
        values = jnp.concatenate(split(cells[pl.ds(i * step, step)].reshape(step * cols, depth)), axis=1)
        both = dot(table[...], values, ((1,), (1,)))
        result = both[:depth] + both[depth:]
        for row in range(step):
            piece = result[:, row * cols : (row + 1) * cols]
            at = pl.multiple_of(i * (step * 8) + row * 8, 8)
            out[:, :, pl.ds(at, 8), :] = piece.reshape(groups, parts, 8, cols)
        return carry

    lax.fori_loop(0, rows // step, body, 0)


def depth_out_kernel(table_ref, spec_ref, out_ref, held, sem):
    rows, cols, depth = out_ref.shape
    count = sem.shape[0]
    step = rows // count

    def copy(i):
        at = pl.ds(i * step, step)
        return pltpu.make_async_copy(held.at[at], out_ref.at[at], sem.at[i])

    def body(i, carry):
        pieces = [
            spec_ref[:, :, pl.ds(pl.multiple_of((i * step + row) * 8, 8), 8), :].reshape(depth, cols) for row in range(step)
        ]
        values = jnp.concatenate(split(jnp.concatenate(pieces, axis=1)), axis=0)
        both = dot(values, table_ref[...], ((0,), (0,)))
        held[pl.ds(i * step, step)] = (both[:, :depth] + both[:, depth:]).reshape(step, cols, depth)
        copy(i).start()
        return carry

    lax.fori_loop(0, count, body, 0)

    def finish(i, carry):
        copy(i).wait()
        return carry

    lax.fori_loop(0, count, finish, 0)


def green_terms(green_ref):
    count = green_ref.shape[0] // 64
    rest = jnp.concatenate([green_ref[pl.ds(k2, 64, stride=count), :] for k2 in range(count)], axis=0)
    terms = []
    for _ in range(3):
        terms.append(rest.astype(bf16))
        rest = rest - terms[-1].astype(f32)
    return jnp.concatenate(terms[:2], axis=1), terms[2]


def pick_green(part, pick_ref, terms, out_ref):
    groups, parts, halves, rows, _ = out_ref.shape
    size = groups * halves * 8
    pick = pick_ref[part * 2 * size : (part + 1) * 2 * size, :]
    first, last = terms
    result = dot(jnp.concatenate([pick, pick], axis=1), first, ((1,), (1,))) + dot(pick, last, ((1,), (1,)))
    first_lanes = lax.broadcasted_iota(jnp.int32, (size, 128), 1) < 64
    place = lax.rem(lax.broadcasted_iota(jnp.int32, (size, 128), 0), 8) // 2
    for tile in range(rows // 8):
        spread = []
        for pair in (2 * tile, 2 * tile + 1):
            own = result[:size, pair * 128 : (pair + 1) * 128]
            mirror = result[size:, pair * 128 : (pair + 1) * 128]
            spread.append(jnp.where(first_lanes, own, pltpu.roll(mirror, 64, 1)))
            spread.append(jnp.where(first_lanes, pltpu.roll(own, 64, 1), mirror))
        packed = jnp.where(place < 2, jnp.where(place < 1, spread[0], spread[1]), jnp.where(place < 3, spread[2], spread[3]))
        out_ref[:, part, :, tile * 8 : (tile + 1) * 8, :] = packed.reshape(groups, halves, 8, 128)


def planes_kernel(
    gy_count, gz_count, reps,
    cells_in, green_in, pick_in, depth_table, waves_ref, flips_ref, home_ref,
    cells_ref, field_ref, pick_ref, depth_ref, gains_ref, spec_ref,
    planes, green, freq, tables, flips,
    fwd_send, fwd_recv, back_send, back_recv, green_send, green_recv, right_send, left_send, line_recv, own_sem, table_sem, in_sem,
):
    groups = gy_count * gz_count
    rep, gy, gz = lax.axis_index("rep"), lax.axis_index("gy"), lax.axis_index("gz")
    slot = gy * gz_count + gz
    rows = spec_ref.shape[2] // 8
    ng = flips_ref.shape[0]
    piece = gains_ref.shape[3]
    quarters = [(part, half) for part in range(PARTS) for half in range(HALVES)]

    def partner(step):
        there_y = lax.rem(gy + step // gz_count, gy_count)
        there_z = lax.rem(gz + step % gz_count, gz_count)
        return there_y * gz_count + there_z, {"rep": rep, "gy": there_y, "gz": there_z}

    def along(step):
        return {"rep": lax.rem(rep + step + reps, reps), "gy": gy, "gz": gz}

    inputs = [
        pltpu.make_async_copy(source, held, in_sem.at[i])
        for i, (source, held) in enumerate((
            (green_in, field_ref), (pick_in, pick_ref), (cells_in, cells_ref), (depth_table, depth_ref)))
    ]
    for copy in inputs:
        copy.start()

    loads = []
    for table, swap in enumerate((False, True, False, True)):
        minus, plus = (1, 2) if swap else (2, 1)
        for quadrant, wave in enumerate((0, minus, plus, 0)):
            loads.append(pltpu.make_async_copy(
                waves_ref.at[wave],
                tables.at[table, :, pl.ds(quadrant // 2 * ng, ng), pl.ds(quadrant % 2 * ng, ng)],
                table_sem.at[4 * table + quadrant]))
    loads.append(pltpu.make_async_copy(flips_ref, flips, table_sem.at[16]))
    for load in loads:
        load.start()

    order = sorted(range(1, groups), key=lambda s: (-(s % gz_count), s))

    barrier = pltpu.get_barrier_semaphore()
    for step in order:
        pl.semaphore_signal(barrier, inc=1, device_id=partner(step)[1], device_id_type=MESH)

    @pl.when(rep + 1 < reps)
    def _():
        pl.semaphore_signal(barrier, inc=1, device_id=along(1), device_id_type=MESH)

    @pl.when(rep >= 1)
    def _():
        pl.semaphore_signal(barrier, inc=1, device_id=along(-1), device_id_type=MESH)

    for copy in inputs[:2]:
        copy.wait()
    terms = green_terms(field_ref)
    pick_green(0, pick_ref, terms, gains_ref)
    pl.semaphore_wait(barrier, groups - 1 + lax.div(rep + reps - 1, reps) + lax.div(2 * reps - 2 - rep, reps))

    def green_copy(step, source, part, half):
        there, device = partner(step)
        return pltpu.make_async_remote_copy(
            src_ref=gains_ref.at[there, part, half], dst_ref=green.at[rep, part, half, pl.ds(source * piece, piece), :],
            send_sem=green_send.at[there, part, half], recv_sem=green_recv.at[source, part, half],
            device_id=device, device_id_type=MESH)

    def fwd_copy(step, source, part):
        there, device = partner(step)
        return pltpu.make_async_remote_copy(
            src_ref=spec_ref.at[there, part], dst_ref=planes.at[source, part],
            send_sem=fwd_send.at[there, part], recv_sem=fwd_recv.at[source, part], device_id=device, device_id_type=MESH)

    def back_copy(step, source, part):
        there, device = partner(step)
        return pltpu.make_async_remote_copy(
            src_ref=planes.at[there, part], dst_ref=home_ref.at[source, part],
            send_sem=back_send.at[there, part], recv_sem=back_recv.at[source, part], device_id=device, device_id_type=MESH)

    def line_copy(block, at, sem, step):
        return pltpu.make_async_remote_copy(
            src_ref=green.at[(block, *at)], dst_ref=green.at[(block, *at)], send_sem=sem.at[at],
            recv_sem=line_recv.at[(block, *at)], device_id=along(step), device_id_type=MESH)

    own_green = {
        (part, half): pltpu.make_async_copy(
            gains_ref.at[slot, part, half], green.at[rep, part, half, pl.ds(slot * piece, piece), :],
            own_sem.at[PARTS + part * HALVES + half])
        for part, half in quarters
    }
    own_planes = [pltpu.make_async_copy(spec_ref.at[slot, h], planes.at[slot, h], own_sem.at[h]) for h in range(PARTS)]

    def green_start(part):
        for half in range(HALVES):
            for step in order:
                green_copy(step, slot, part, half).start()

    green_start(0)
    for part in range(1, PARTS):
        pick_green(part, pick_ref, terms, gains_ref)
        green_start(part)
    for at in quarters:
        own_green[at].start()
    for copy in inputs[2:]:
        copy.wait()
    depth_in(depth_ref, cells_ref, spec_ref)
    for part in range(PARTS):
        for step in order:
            fwd_copy(step, slot, part).start()
    for copy in own_planes:
        copy.start()

    def green_wait(at):
        own_green[at].wait()
        for step in order:
            green_copy(step, partner(step)[0], *at).wait_recv()

    def line_start(at, hop=None):
        right, left = rep + 1 < reps, rep >= 1
        if hop is not None:
            right, left = right & (rep == hop), left & (rep + hop == reps - 1)

        @pl.when(right)
        def _():
            line_copy(rep, at, right_send.at[0], 1).start()

        @pl.when(left)
        def _():
            line_copy(rep, at, left_send.at[0], -1).start()

    def relay(hop, at):
        @pl.when((rep >= hop) & (rep + 1 < reps))
        def _():
            line_copy(rep - hop, at, right_send.at[hop], 1).wait_recv()
            line_copy(rep - hop, at, right_send.at[hop], 1).start()

        @pl.when((rep + hop < reps) & (rep >= 1))
        def _():
            line_copy(rep + hop, at, left_send.at[hop], -1).wait_recv()
            line_copy(rep + hop, at, left_send.at[hop], -1).start()

    def line_end(at):
        for hop in range(1, reps):
            @pl.when(rep + 1 == reps)
            def _():
                line_copy(rep - hop, at, right_send.at[hop], 1).wait_recv()

            @pl.when(rep == 0)
            def _():
                line_copy(rep + hop, at, left_send.at[hop], -1).wait_recv()

    def load_plane(part, row):
        bands = []
        for y in range(gy_count):
            bands.append(jnp.concatenate(
                [planes[y * gz_count + x, part, pl.ds(row, rows, stride=8), :] for x in range(gz_count)], axis=0))
        return jnp.concatenate(bands, axis=1)

    def forward(part):
        def body(p, carry):
            values = jnp.concatenate([load_plane(part, p), load_plane(part, 4 + p)], axis=1)
            inner = dot_table(values, tables[0, 0], tables[0, 1])
            inner = jnp.concatenate([inner[:, :ng], inner[:, ng:]], axis=0)
            freq[part * 4 + p] = table_dot(tables[1, 0], tables[1, 1], inner)
            return carry

        lax.fori_loop(0, 4, body, 0)

    def reflect_plane(values):
        high, low = split(values)
        turned = dot(flips[...], high) + dot(flips[...], low)
        high, low = split(turned)
        return dot(high, flips[...]) + dot(low, flips[...])

    def backward(part, half):
        def body(p, carry):
            row = half * 2 + p
            plane = part * 4 + row
            own, mirror = [], []
            lane = lax.broadcasted_iota(jnp.int32, (ng, 128), 1)
            for r in range(0, reps, 2):
                one, two = (green[q, part, half, pl.ds(p, ng, stride=2), :] for q in (r, r + 1))
                own.append(jnp.where(lane < 64, one, pltpu.roll(two, 64, 1)))
                mirror.append(jnp.where(lane < 64, pltpu.roll(one, 64, 1), two))
            own = jnp.concatenate(own, axis=1).T
            mirror = jnp.concatenate(mirror, axis=1).T
            packed = (slot == 0) & (plane == 0)

            @pl.when(jnp.logical_not(packed))
            def _():
                gain = 0.5 * (own + reflect_plane(mirror))
                freq[plane] = freq[plane] * jnp.concatenate([gain, gain], axis=0)

            @pl.when(packed)
            def _():
                first = 0.5 * (own + reflect_plane(own))
                second = 0.5 * (mirror + reflect_plane(mirror))
                mean, odd = 0.5 * (first + second), 0.5 * (first - second)
                real, imag = freq[plane, :ng, :], freq[plane, ng:, :]
                freq[plane, :ng, :] = real * mean + reflect_plane(real) * odd
                freq[plane, ng:, :] = imag * mean - reflect_plane(imag) * odd

            undo = table_dot(tables[2, 0], tables[2, 1], freq[plane])
            undo = jnp.concatenate([undo[:ng], undo[ng:]], axis=1)
            cells = dot_table(undo, tables[3, 0], tables[3, 1])
            cols = ng // gy_count
            for c in range(2):
                for y in range(gy_count):
                    for x in range(gz_count):
                        planes[y * gz_count + x, part, pl.ds(c * 4 + row, rows, stride=8), :] = cells[
                            x * rows : (x + 1) * rows, c * ng + y * cols : c * ng + (y + 1) * cols]
            return carry

        lax.fori_loop(0, 2, body, 0)

    own_home = [pltpu.make_async_copy(planes.at[slot, h], home_ref.at[slot, h], own_sem.at[h]) for h in range(PARTS)]

    def arrive(part):
        own_planes[part].wait()
        for step in order:
            fwd_copy(step, partner(step)[0], part).wait_recv()
        forward(part)

    def depart(part):
        for step in order:
            back_copy(step, slot, part).start()
        own_home[part].start()

    first, second = quarters[:HALVES], quarters[HALVES:]

    def second_start(hop):
        for at in second:
            line_start(at, hop)

    for at in first:
        green_wait(at)
        line_start(at)
    relay(1, first[0])
    for at in second:
        green_wait(at)
    second_start(0)
    relay(1, first[1])
    second_start(1)
    for hop in range(2, reps - 1):
        for at in first:
            relay(hop, at)
        second_start(hop)
    for load in loads:
        load.wait()
    relay(1, second[0])
    arrive(0)
    relay(1, second[1])
    for at in first:
        line_end(at)
        for hop in range(2, reps - 1):
            relay(hop, second[at[1]])
        backward(*at)
    depart(0)
    arrive(1)
    for at in second:
        line_end(at)
        backward(*at)
    depart(1)

    for part in range(PARTS):
        for step in order:
            fwd_copy(step, slot, part).wait_send()
    for at in quarters:
        for step in order:
            green_copy(step, slot, *at).wait_send()
        for hop in range(reps):
            @pl.when((rep >= hop) & (rep + 1 < reps))
            def _():
                line_copy(rep - hop, at, right_send.at[hop], 1).wait_send()

            @pl.when((rep + hop < reps) & (rep >= 1))
            def _():
                line_copy(rep + hop, at, left_send.at[hop], -1).wait_send()
    for part in range(PARTS):
        own_home[part].wait()
        for step in order:
            back_copy(step, slot, part).wait_send()
            back_copy(step, partner(step)[0], part).wait_recv()


def fused_plan(charges, green):
    gy_count, gz_count, reps = lax.axis_size("gy"), lax.axis_size("gz"), lax.axis_size("rep")
    groups = gy_count * gz_count
    rows, cols, depth = charges.shape
    ng = rows * gz_count
    half = depth // 2
    each = half // groups
    forward_table, back_table = depth_tables(depth, groups, each)
    chunks = rows // 16
    spec_shape = jax.ShapeDtypeStruct((groups, PARTS, rows * 8, cols), f32)

    k1, k2, _ = green.shape
    own_index = np.arange(half)
    opposite = np.where(own_index == 0, half, depth - own_index)
    quad, place = np.divmod(np.arange(groups * HALVES * 8), 8)
    quad = quad // HALVES * PARTS * HALVES + quad % HALVES
    pick = []
    for part in range(PARTS):
        bins = (quad + part * HALVES) * 2 + place % 2
        pick += [own_index[bins], opposite[bins]]
    pick = (np.concatenate(pick)[:, None] == np.arange(depth)[None, :]).astype(np.float32)
    index = np.arange(ng)
    angle = 2.0 * np.pi * ((index[:, None] * index[None, :]) % ng) / ng
    cos, sin = np.cos(angle), np.sin(angle)
    waves = stacked_table(np.stack([cos, sin, -sin]), 1)
    flips = jnp.asarray((index[:, None] + index[None, :]) % ng == 0, bf16)

    dma = pltpu.SemaphoreType.DMA
    both, lines = (groups, PARTS), (reps, PARTS, HALVES)
    home = pl.pallas_call(
        functools.partial(planes_kernel, gy_count, gz_count, reps),
        out_shape=spec_shape, name="planes",
        in_specs=[pl.BlockSpec(memory_space=pl.ANY)] * 6, out_specs=pl.BlockSpec(memory_space=pl.ANY),
        scratch_shapes=[
            pltpu.VMEM(charges.shape, f32),
            pltpu.VMEM((k1 * k2, depth), f32),
            pltpu.VMEM(pick.shape, bf16),
            pltpu.VMEM((2 * depth, 2 * depth), bf16),
            pltpu.VMEM((groups, PARTS, HALVES, k2 * 2, 2 * k1), f32),
            pltpu.VMEM(spec_shape.shape, f32),
            pltpu.VMEM(spec_shape.shape, f32),
            pltpu.VMEM((reps, PARTS, HALVES, ng * 2, 2 * k1), f32),
            pltpu.VMEM((each, 2 * ng, ng), f32),
            pltpu.VMEM((4, 2, 2 * ng, 2 * ng), bf16),
            pltpu.VMEM((ng, ng), bf16),
            dma(both), dma(both), dma(both), dma(both), dma((*both, HALVES)), dma((*both, HALVES)),
            dma(lines), dma(lines), dma(lines), dma((PARTS * (1 + HALVES),)), dma((17,)), dma((4,)),
        ],
        compiler_params=pltpu.CompilerParams(
            collective_id=0, has_side_effects=True, vmem_limit_bytes=44 * 2**20),
    )(*(
        pltpu.with_memory_space_constraint(value, pltpu.HBM)
        for value in (
            charges, green.reshape(k1 * k2, depth), jnp.asarray(pick, bf16), wide_table(forward_table, 0), waves, flips)
    ))

    vmem = pl.BlockSpec(memory_space=pltpu.VMEM)
    return pl.pallas_call(
        depth_out_kernel, out_shape=jax.ShapeDtypeStruct(charges.shape, f32), name="depth_out",
        in_specs=[vmem, vmem], out_specs=pl.BlockSpec(memory_space=pl.ANY),
        scratch_shapes=[pltpu.VMEM(charges.shape, f32), dma((chunks,))],
        compiler_params=pltpu.CompilerParams(vmem_limit_bytes=16 * 2**20),
    )(wide_table(back_table / (ng * ng * depth), 1), home)


def on_device(charges, green):
    groups = lax.axis_size("gy") * lax.axis_size("gz")
    rows, cols, depth = charges.shape
    aligned = (
        cols % 128 == 0 and depth % 128 == 0 and depth == 16 * groups and rows % 8 == 0
        and green.shape[0] == 64 and lax.axis_size("rep") % 2 == 0 and lax.axis_size("rep") > 2
        and rows * lax.axis_size("gz") == cols * lax.axis_size("gy")
    )
    return fused_plan(charges, green) if aligned else slab_plan(charges, green)


def solution(mesh):
    placed = (P(("rep", "gz"), "gy", None), P("rep", ("gy", "gz"), None))
    return jax.shard_map(
        on_device,
        mesh=mesh,
        in_specs=placed,
        out_specs=P(("rep", "gz"), "gy", None),
        check_vma=False,
    )
```

```python
import functools
import math

import jax
import jax.numpy as jnp
import numpy as np
from jax import lax
from jax.experimental import pallas as pl
from jax.experimental.pallas import tpu as pltpu
from jax.sharding import PartitionSpec as P

NG = 256
NZ = 128


two_pi = 2.0 * math.pi
highest = lax.Precision.HIGHEST


def tables(length, rows_index, cols_index):
    phase = rows_index[:, None] * cols_index[None, :] % length
    angle = phase.astype(jnp.float32) * (two_pi / length)
    return (jnp.cos(angle), jnp.sin(angle))


def reflect(values):
    return jnp.roll(jnp.flip(values, (1, 2)), (1, 1), axis=(1, 2))


def slab_plan(charges, green):
    gy_count = lax.axis_size("gy")
    gz_count = lax.axis_size("gz")
    groups = gy_count * gz_count
    half = NZ // 2
    per_device = half // groups
    col_block = charges.shape[1]
    depth = jnp.arange(NZ, dtype=jnp.int32)
    bins = jnp.arange(half, dtype=jnp.int32)
    indices = jnp.arange(NG, dtype=jnp.int32)
    cos_depth, sin_depth = tables(NZ, depth, bins)
    alternate = (1 - 2 * (depth % 2)).astype(jnp.float32)
    sin_packed = jnp.where(bins[None, :] == 0, -alternate[:, None], sin_depth)
    spec_re = jnp.einsum("xyz,zk->kxy", charges, cos_depth, precision=highest)
    spec_im = -jnp.einsum("xyz,zk->kxy", charges, sin_packed, precision=highest)
    own = jnp.moveaxis(green[:, :, :half], 2, 0)
    mirror = jnp.concatenate(
        [green[:, :, half : half + 1], jnp.flip(green[:, :, half + 1 :], 2)], axis=2
    )
    mirror = jnp.moveaxis(mirror, 2, 0)
    own, mirror = (
        lax.all_to_all(own, ("gy", "gz"), split_axis=0, concat_axis=2, tiled=True),
        lax.all_to_all(mirror, ("gy", "gz"), split_axis=0, concat_axis=2, tiled=True),
    )
    own, mirror = (
        lax.all_gather(own, "rep", axis=1, tiled=True),
        lax.all_gather(mirror, "rep", axis=1, tiled=True),
    )
    plane_re, plane_im = (
        lax.all_to_all(spec_re, ("gy", "gz"), split_axis=0, concat_axis=1, tiled=True),
        lax.all_to_all(spec_im, ("gy", "gz"), split_axis=0, concat_axis=1, tiled=True),
    )
    plane_re = plane_re.reshape(per_device, gy_count, NG, col_block)
    plane_im = plane_im.reshape(per_device, gy_count, NG, col_block)
    cos_plain, sin_plain = tables(NG, indices, indices)
    wide_cos = cos_plain.reshape(NG, gy_count, col_block)
    wide_sin = sin_plain.reshape(NG, gy_count, col_block)

    def second_in(matrix, values):
        return jnp.einsum("kgc,bgxc->bxk", matrix, values, precision=highest)

    def first_in(matrix, values):
        return jnp.einsum("kx,bxj->bkj", matrix, values, precision=highest)

    inner_re = second_in(wide_cos, plane_re) + second_in(wide_sin, plane_im)
    inner_im = second_in(wide_cos, plane_im) - second_in(wide_sin, plane_re)
    freq_re = first_in(cos_plain, inner_re) + first_in(sin_plain, inner_im)
    freq_im = first_in(cos_plain, inner_im) - first_in(sin_plain, inner_re)
    slot = lax.axis_index("gy") * gz_count + lax.axis_index("gz")
    packed = ((slot == 0) & (jnp.arange(per_device) == 0))[:, None, None]
    plain_gain = 0.5 * (own + reflect(mirror))
    first_gain = jnp.where(packed, 0.5 * (own + reflect(own)), plain_gain)
    second_gain = jnp.where(packed, 0.5 * (mirror + reflect(mirror)), plain_gain)
    mean_gain = 0.5 * (first_gain + second_gain)
    odd_gain = 0.5 * (first_gain - second_gain)
    prod_re = freq_re * mean_gain + reflect(freq_re) * odd_gain
    prod_im = freq_im * mean_gain - reflect(freq_im) * odd_gain
    undo_re = first_in(cos_plain, prod_re) - first_in(sin_plain, prod_im)
    undo_im = first_in(sin_plain, prod_re) + first_in(cos_plain, prod_im)

    def second_out(matrix, values):
        return jnp.einsum("kgc,bxk->bgxc", matrix, values, precision=highest)

    cells_re = second_out(wide_cos, undo_re) - second_out(wide_sin, undo_im)
    cells_im = second_out(wide_sin, undo_re) + second_out(wide_cos, undo_im)
    cells_re = cells_re.reshape(per_device, gy_count * NG, col_block)
    cells_im = cells_im.reshape(per_device, gy_count * NG, col_block)
    home_re, home_im = (
        lax.all_to_all(cells_re, ("gy", "gz"), split_axis=1, concat_axis=0, tiled=True),
        lax.all_to_all(cells_im, ("gy", "gz"), split_axis=1, concat_axis=0, tiled=True),
    )
    weight = jnp.where(bins == 0, 1.0, 2.0).astype(jnp.float32)
    cos_back = (cos_depth * weight[None, :]).T
    sin_back = jnp.where(bins[:, None] == 0, alternate[None, :], -2.0 * sin_depth.T)
    result_field = jnp.einsum("kxy,kz->xyz", home_re, cos_back, precision=highest)
    result_field = result_field + jnp.einsum("kxy,kz->xyz", home_im, sin_back, precision=highest)
    return result_field / (NG * NG * NZ)


f32 = jnp.float32
bf16 = jnp.bfloat16
MESH = pl.DeviceIdType.MESH
PARTS = 2
HALVES = 2


def split(values):
    high = values.astype(bf16)
    return high, (values - high.astype(f32)).astype(bf16)


def stacked_table(table, axis):
    rounded = table.astype(jnp.bfloat16)
    return jnp.asarray(np.stack([rounded, (table - rounded.astype(np.float64)).astype(jnp.bfloat16)], axis=axis))


def dot(left, right, dims=((1,), (0,))):
    return lax.dot_general(left, right, (dims, ((), ())), preferred_element_type=f32)


def dot_table(values, table_high, table_low, dims=((1,), (0,))):
    high, low = split(values)
    return dot(high, table_high, dims) + (dot(low, table_high, dims) + dot(high, table_low, dims))


def table_dot(table_high, table_low, values, dims=((1,), (0,))):
    high, low = split(values)
    return dot(table_high, high, dims) + (dot(table_high, low, dims) + dot(table_low, high, dims))


def depth_tables(length, groups, bins_each):
    per_part = bins_each // PARTS
    forward, back = [], []
    z = np.arange(length)
    alternate = 1.0 - 2.0 * (z % 2)
    for start in range(0, groups * bins_each, per_part):
        for imaginary in (False, True):
            for k in range(start, start + per_part):
                angle = 2.0 * np.pi * ((k * z) % length) / length
                if k == 0:
                    forward.append(alternate if imaginary else np.ones(length))
                    back.append(alternate if imaginary else np.ones(length))
                else:
                    forward.append(-np.sin(angle) if imaginary else np.cos(angle))
                    back.append(-2.0 * np.sin(angle) if imaginary else 2.0 * np.cos(angle))
    return np.stack(forward), np.stack(back)


def wide_table(table, axis):
    rounded = table.astype(jnp.bfloat16)
    low = (table - rounded.astype(np.float64)).astype(jnp.bfloat16)
    both = np.concatenate([rounded, rounded], axis=1 - axis)
    return jnp.asarray(np.concatenate([both, np.concatenate([low, np.zeros_like(low)], axis=1 - axis)], axis=axis))


def depth_in(table, cells, out):
    groups, parts, _, cols = out.shape
    rows, depth, step = cells.shape[0], cells.shape[2], 8

    def body(i, carry):
        values = jnp.concatenate(split(cells[pl.ds(i * step, step)].reshape(step * cols, depth)), axis=1)
        both = dot(table[...], values, ((1,), (1,)))
        result = both[:depth] + both[depth:]
        for row in range(step):
            piece = result[:, row * cols : (row + 1) * cols]
            at = pl.multiple_of(i * (step * 8) + row * 8, 8)
            out[:, :, pl.ds(at, 8), :] = piece.reshape(groups, parts, 8, cols)
        return carry

    lax.fori_loop(0, rows // step, body, 0)


def depth_out_kernel(table_ref, spec_ref, out_ref, held, sem):
    rows, cols, depth = out_ref.shape
    count = sem.shape[0]
    step = rows // count

    def copy(i):
        at = pl.ds(i * step, step)
        return pltpu.make_async_copy(held.at[at], out_ref.at[at], sem.at[i])

    def body(i, carry):
        pieces = [
            spec_ref[:, :, pl.ds(pl.multiple_of((i * step + row) * 8, 8), 8), :].reshape(depth, cols) for row in range(step)
        ]
        values = jnp.concatenate(split(jnp.concatenate(pieces, axis=1)), axis=0)
        both = dot(values, table_ref[...], ((0,), (0,)))
        held[pl.ds(i * step, step)] = (both[:, :depth] + both[:, depth:]).reshape(step, cols, depth)
        copy(i).start()
        return carry

    lax.fori_loop(0, count, body, 0)

    def finish(i, carry):
        copy(i).wait()
        return carry

    lax.fori_loop(0, count, finish, 0)


def green_terms(count, green_ref):
    size, pitch, lanes = green_ref.shape
    flat = green_ref.reshape(size * pitch, lanes)
    rest = jnp.concatenate([flat[pl.ds(k2, size, stride=pitch), :] for k2 in range(count)], axis=0)
    terms = []
    for _ in range(3):
        terms.append(rest.astype(bf16))
        rest = rest - terms[-1].astype(f32)
    return jnp.concatenate(terms[:2], axis=1), terms[2]


def pick_green(part, pick_ref, terms, out_ref):
    groups, parts, halves, rows, _ = out_ref.shape
    size = groups * halves * 8
    pick = pick_ref[part * 2 * size : (part + 1) * 2 * size, :]
    first, last = terms
    result = dot(jnp.concatenate([pick, pick], axis=1), first, ((1,), (1,))) + dot(pick, last, ((1,), (1,)))
    first_lanes = lax.broadcasted_iota(jnp.int32, (size, 128), 1) < 64
    place = lax.rem(lax.broadcasted_iota(jnp.int32, (size, 128), 0), 8) // 2
    for tile in range(rows // 8):
        spread = []
        for pair in (2 * tile, 2 * tile + 1):
            own = result[:size, pair * 128 : (pair + 1) * 128]
            mirror = result[size:, pair * 128 : (pair + 1) * 128]
            spread.append(jnp.where(first_lanes, own, pltpu.roll(mirror, 64, 1)))
            spread.append(jnp.where(first_lanes, pltpu.roll(own, 64, 1), mirror))
        packed = jnp.where(place < 2, jnp.where(place < 1, spread[0], spread[1]), jnp.where(place < 3, spread[2], spread[3]))
        out_ref[:, part, :, tile * 8 : (tile + 1) * 8, :] = packed.reshape(groups, halves, 8, 128)


def planes_kernel(
    gy_count, gz_count, reps,
    cells_in, green_in, pick_in, depth_table, waves_ref, flips_ref, home_ref,
    cells_ref, field_ref, pick_ref, depth_ref, gains_ref, spec_ref,
    planes, green, freq, tables, flips,
    fwd_send, fwd_recv, back_send, back_recv, green_send, green_recv, right_send, left_send, line_recv, own_sem, table_sem, in_sem,
):
    groups = gy_count * gz_count
    rep, gy, gz = lax.axis_index("rep"), lax.axis_index("gy"), lax.axis_index("gz")
    slot = gy * gz_count + gz
    rows = spec_ref.shape[2] // 8
    ng = flips_ref.shape[0]
    piece = gains_ref.shape[3]
    quarters = [(part, half) for part in range(PARTS) for half in range(HALVES)]

    def partner(step):
        there_y = lax.rem(gy + step // gz_count, gy_count)
        there_z = lax.rem(gz + step % gz_count, gz_count)
        return there_y * gz_count + there_z, {"rep": rep, "gy": there_y, "gz": there_z}

    def along(step):
        return {"rep": lax.rem(rep + step + reps, reps), "gy": gy, "gz": gz}

    inputs = [
        pltpu.make_async_copy(source, held, in_sem.at[i])
        for i, (source, held) in enumerate((
            (green_in, field_ref.at[:, pl.ds(0, green_in.shape[1]), :]), (pick_in, pick_ref), (cells_in, cells_ref), (depth_table, depth_ref)))
    ]
    for copy in inputs[:2]:
        copy.start()

    loads = []
    for table, swap in enumerate((False, True)):
        minus, plus = (1, 2) if swap else (2, 1)
        for quadrant, wave in enumerate((0, minus, plus, 0)):
            loads.append(pltpu.make_async_copy(
                waves_ref.at[wave],
                tables.at[table, :, pl.ds(quadrant // 2 * ng, ng), pl.ds(quadrant % 2 * ng, ng)],
                table_sem.at[4 * table + quadrant]))
    loads.append(pltpu.make_async_copy(flips_ref, flips, table_sem.at[8]))

    order = sorted(range(1, groups), key=lambda s: (-(s % gz_count), s))

    barrier = pltpu.get_barrier_semaphore()
    for step in order:
        pl.semaphore_signal(barrier, inc=1, device_id=partner(step)[1], device_id_type=MESH)

    @pl.when(rep + 1 < reps)
    def _():
        pl.semaphore_signal(barrier, inc=1, device_id=along(1), device_id_type=MESH)

    @pl.when(rep >= 1)
    def _():
        pl.semaphore_signal(barrier, inc=1, device_id=along(-1), device_id_type=MESH)

    for copy in inputs[:2]:
        copy.wait()
    for copy in inputs[2:]:
        copy.start()
    terms = green_terms(green_in.shape[1], field_ref)
    pick_green(0, pick_ref, terms, gains_ref)
    pl.semaphore_wait(barrier, groups - 1 + lax.div(rep + reps - 1, reps) + lax.div(2 * reps - 2 - rep, reps))

    def green_copy(step, source, part, half):
        there, device = partner(step)
        return pltpu.make_async_remote_copy(
            src_ref=gains_ref.at[there, part, half], dst_ref=green.at[rep, part, half, pl.ds(source * piece, piece), :],
            send_sem=green_send.at[0], recv_sem=green_recv.at[part, half],
            device_id=device, device_id_type=MESH)

    def fwd_copy(step, source, part):
        there, device = partner(step)
        return pltpu.make_async_remote_copy(
            src_ref=spec_ref.at[there, part], dst_ref=planes.at[source, part],
            send_sem=fwd_send.at[0], recv_sem=fwd_recv.at[part], device_id=device, device_id_type=MESH)

    def back_copy(step, source, part):
        there, device = partner(step)
        return pltpu.make_async_remote_copy(
            src_ref=planes.at[there, part], dst_ref=home_ref.at[source, part],
            send_sem=back_send.at[0], recv_sem=back_recv.at[0], device_id=device, device_id_type=MESH)

    def whole(ref, sem):
        return pltpu.make_async_remote_copy(
            src_ref=ref, dst_ref=ref, send_sem=sem, recv_sem=sem, device_id=partner(1)[1], device_id_type=MESH)

    def line_copy(block, at, sem, step):
        return pltpu.make_async_remote_copy(
            src_ref=green.at[(block, *at)], dst_ref=green.at[(block, *at)], send_sem=sem,
            recv_sem=line_recv.at[(block, *at)], device_id=along(step), device_id_type=MESH)

    def green_start(part):
        for half in range(HALVES):
            for step in order:
                green_copy(step, slot, part, half).start()

    green_start(0)
    for part in range(1, PARTS):
        pick_green(part, pick_ref, terms, gains_ref)
        green_start(part)
    for part, half in quarters:
        green[rep, part, half, pl.ds(slot * piece, piece), :] = gains_ref[slot, part, half]
    for copy in inputs[2:]:
        copy.wait()
    for load in loads:
        load.start()
    depth_in(depth_ref, cells_ref, spec_ref)
    for part in range(PARTS):
        for step in order:
            fwd_copy(step, slot, part).start()
    planes[slot] = spec_ref[slot]
    others = pl.ds(0, groups - 1)

    def green_wait(at):
        whole(green.at[(rep, *at, pl.ds(0, (groups - 1) * piece))], green_recv.at[at]).wait_recv()

    def line_start(at, hop=None):
        right, left = rep + 1 < reps, rep >= 1
        if hop is not None:
            right, left = right & (rep == hop), left & (rep + hop == reps - 1)

        @pl.when(right)
        def _():
            line_copy(rep, at, right_send.at[0], 1).start()

        @pl.when(left)
        def _():
            line_copy(rep, at, left_send.at[0], -1).start()

    def relay(hop, at):
        @pl.when((rep >= hop) & (rep + 1 < reps))
        def _():
            line_copy(rep - hop, at, right_send.at[hop], 1).wait_recv()
            line_copy(rep - hop, at, right_send.at[hop], 1).start()

        @pl.when((rep + hop < reps) & (rep >= 1))
        def _():
            line_copy(rep + hop, at, left_send.at[hop], -1).wait_recv()
            line_copy(rep + hop, at, left_send.at[hop], -1).start()

    def line_end(at):
        for hop in range(1, reps):
            @pl.when(rep + 1 == reps)
            def _():
                line_copy(rep - hop, at, right_send.at[hop], 1).wait_recv()

            @pl.when(rep == 0)
            def _():
                line_copy(rep + hop, at, left_send.at[hop], -1).wait_recv()

    def load_plane(part, row):
        bands = []
        for y in range(gy_count):
            bands.append(jnp.concatenate(
                [planes[y * gz_count + x, part, pl.ds(row, rows, stride=8), :] for x in range(gz_count)], axis=0))
        return jnp.concatenate(bands, axis=1)

    def forward(part):
        def body(p, carry):
            values = jnp.concatenate([load_plane(part, p), load_plane(part, 4 + p)], axis=1)
            inner = dot_table(values, tables[0, 0], tables[0, 1])
            inner = jnp.concatenate([inner[:, :ng], inner[:, ng:]], axis=0)
            freq[part * 4 + p] = table_dot(tables[1, 0], tables[1, 1], inner)
            return carry

        lax.fori_loop(0, 4, body, 0)

    def reflect_plane(values):
        high, low = split(values)
        turned = dot(flips[...], high) + dot(flips[...], low)
        high, low = split(turned)
        return dot(high, flips[...]) + dot(low, flips[...])

    def backward(part, half):
        def body(p, carry):
            row = half * 2 + p
            plane = part * 4 + row
            own, mirror = [], []
            lane = lax.broadcasted_iota(jnp.int32, (ng, 128), 1)
            for r in range(0, reps, 2):
                one, two = (green[q, part, half, pl.ds(p, ng, stride=2), :] for q in (r, r + 1))
                own.append(jnp.where(lane < 64, one, pltpu.roll(two, 64, 1)))
                mirror.append(jnp.where(lane < 64, pltpu.roll(one, 64, 1), two))
            own = jnp.concatenate(own, axis=1).T
            mirror = jnp.concatenate(mirror, axis=1).T
            packed = (slot == 0) & (plane == 0)

            @pl.when(jnp.logical_not(packed))
            def _():
                gain = 0.5 * (own + reflect_plane(mirror))
                freq[plane] = freq[plane] * jnp.concatenate([gain, gain], axis=0)

            @pl.when(packed)
            def _():
                first = 0.5 * (own + reflect_plane(own))
                second = 0.5 * (mirror + reflect_plane(mirror))
                mean, odd = 0.5 * (first + second), 0.5 * (first - second)
                real, imag = freq[plane, :ng, :], freq[plane, ng:, :]
                freq[plane, :ng, :] = real * mean + reflect_plane(real) * odd
                freq[plane, ng:, :] = imag * mean - reflect_plane(imag) * odd

            undo = table_dot(tables[0, 0], tables[0, 1], freq[plane])
            undo = jnp.concatenate([undo[:ng], undo[ng:]], axis=1)
            cells = dot_table(undo, tables[1, 0], tables[1, 1])
            cols = ng // gy_count
            for c in range(2):
                for y in range(gy_count):
                    for x in range(gz_count):
                        planes[y * gz_count + x, part, pl.ds(c * 4 + row, rows, stride=8), :] = cells[
                            x * rows : (x + 1) * rows, c * ng + y * cols : c * ng + (y + 1) * cols]
            return carry

        lax.fori_loop(0, 2, body, 0)

    own_home = [pltpu.make_async_copy(planes.at[slot, h], home_ref.at[slot, h], own_sem.at[h]) for h in range(PARTS)]

    def arrive(part):
        whole(planes.at[others, part], fwd_recv.at[part]).wait_recv()
        forward(part)

    def depart(part):
        for step in order:
            back_copy(step, slot, part).start()
        own_home[part].start()

    first, second = quarters[:HALVES], quarters[HALVES:]

    def second_start(hop):
        for at in second:
            line_start(at, hop)

    for at in first:
        green_wait(at)
        line_start(at)
    relay(1, first[0])
    for at in second:
        green_wait(at)
    second_start(0)
    relay(1, first[1])
    second_start(1)
    for hop in range(2, reps - 1):
        for at in first:
            relay(hop, at)
        second_start(hop)
    for load in loads:
        load.wait()
    relay(1, second[0])
    arrive(0)
    relay(1, second[1])
    for at in first:
        line_end(at)
        backward(*at)
        if at == first[-1]:
            depart(0)
        for hop in range(2, reps - 1):
            relay(hop, second[at[1]])
    arrive(1)
    for at in second:
        line_end(at)
        backward(*at)
    depart(1)

    whole(gains_ref.at[others], green_send.at[0]).wait_send()
    whole(spec_ref.at[others], fwd_send.at[0]).wait_send()
    for hop in range(reps):
        @pl.when((rep >= hop) & (rep + 1 < reps))
        def _():
            whole(green.at[rep - hop], right_send.at[hop]).wait_send()

        @pl.when((rep + hop < reps) & (rep >= 1))
        def _():
            whole(green.at[rep + hop], left_send.at[hop]).wait_send()
    for part in range(PARTS):
        own_home[part].wait()
    whole(planes.at[others], back_send.at[0]).wait_send()
    whole(home_ref.at[others], back_recv.at[0]).wait_recv()


def fused_plan(charges, green):
    gy_count, gz_count, reps = lax.axis_size("gy"), lax.axis_size("gz"), lax.axis_size("rep")
    groups = gy_count * gz_count
    rows, cols, depth = charges.shape
    ng = rows * gz_count
    half = depth // 2
    each = half // groups
    forward_table, back_table = depth_tables(depth, groups, each)
    chunks = rows // 16
    spec_shape = jax.ShapeDtypeStruct((groups, PARTS, rows * 8, cols), f32)

    k1, k2, _ = green.shape
    own_index = np.arange(half)
    opposite = np.where(own_index == 0, half, depth - own_index)
    quad, place = np.divmod(np.arange(groups * HALVES * 8), 8)
    quad = quad // HALVES * PARTS * HALVES + quad % HALVES
    pick = []
    for part in range(PARTS):
        bins = (quad + part * HALVES) * 2 + place % 2
        pick += [own_index[bins], opposite[bins]]
    pick = (np.concatenate(pick)[:, None] == np.arange(depth)[None, :]).astype(np.float32)
    index = np.arange(ng)
    angle = 2.0 * np.pi * ((index[:, None] * index[None, :]) % ng) / ng
    cos, sin = np.cos(angle), np.sin(angle)
    waves = stacked_table(np.stack([cos, sin, -sin]), 1)
    flips = jnp.asarray((index[:, None] + index[None, :]) % ng == 0, bf16)

    dma = pltpu.SemaphoreType.DMA
    home = pl.pallas_call(
        functools.partial(planes_kernel, gy_count, gz_count, reps),
        out_shape=spec_shape, name="planes",
        in_specs=[pl.BlockSpec(memory_space=pl.ANY)] * 6, out_specs=pl.BlockSpec(memory_space=pl.ANY),
        scratch_shapes=[
            pltpu.VMEM(charges.shape, f32),
            pltpu.VMEM((k1, k2 + 8, depth), f32),
            pltpu.VMEM(pick.shape, bf16),
            pltpu.VMEM((2 * depth, 2 * depth), bf16),
            pltpu.VMEM((groups, PARTS, HALVES, k2 * 2, 2 * k1), f32),
            pltpu.VMEM(spec_shape.shape, f32),
            pltpu.VMEM(spec_shape.shape, f32),
            pltpu.VMEM((reps, PARTS, HALVES, ng * 2, 2 * k1), f32),
            pltpu.VMEM((each, 2 * ng, ng), f32),
            pltpu.VMEM((2, 2, 2 * ng, 2 * ng), bf16),
            pltpu.VMEM((ng, ng), bf16),
            dma((1,)), dma((PARTS,)), dma((1,)), dma((1,)), dma((1,)), dma((PARTS, HALVES)),
            dma((reps,)), dma((reps,)), dma((reps, PARTS, HALVES)), dma((PARTS,)), dma((9,)), dma((4,)),
        ],
        compiler_params=pltpu.CompilerParams(
            collective_id=0, has_side_effects=True, vmem_limit_bytes=44 * 2**20),
    )(*(
        pltpu.with_memory_space_constraint(value, pltpu.HBM)
        for value in (
            charges, green, jnp.asarray(pick, bf16), wide_table(forward_table, 0), waves, flips)
    ))

    vmem = pl.BlockSpec(memory_space=pltpu.VMEM)
    return pl.pallas_call(
        depth_out_kernel, out_shape=jax.ShapeDtypeStruct(charges.shape, f32), name="depth_out",
        in_specs=[vmem, vmem], out_specs=pl.BlockSpec(memory_space=pl.ANY),
        scratch_shapes=[pltpu.VMEM(charges.shape, f32), dma((chunks,))],
        compiler_params=pltpu.CompilerParams(vmem_limit_bytes=16 * 2**20),
    )(wide_table(back_table / (ng * ng * depth), 1), home)


def on_device(charges, green):
    groups = lax.axis_size("gy") * lax.axis_size("gz")
    rows, cols, depth = charges.shape
    aligned = (
        cols % 128 == 0 and depth % 128 == 0 and depth == 16 * groups and rows % 8 == 0
        and green.shape[0] == 64 and lax.axis_size("rep") % 2 == 0 and lax.axis_size("rep") > 2
        and rows * lax.axis_size("gz") == cols * lax.axis_size("gy")
    )
    return fused_plan(charges, green) if aligned else slab_plan(charges, green)


def solution(mesh):
    placed = (P(("rep", "gz"), "gy", None), P("rep", ("gy", "gz"), None))
    return jax.shard_map(
        on_device,
        mesh=mesh,
        in_specs=placed,
        out_specs=P(("rep", "gz"), "gy", None),
        check_vma=False,
    )
```

```python
import functools
import math

import jax
import jax.numpy as jnp
import numpy as np
from jax import lax
from jax.experimental import pallas as pl
from jax.experimental.pallas import tpu as pltpu
from jax.sharding import PartitionSpec as P

NG = 256
NZ = 128


two_pi = 2.0 * math.pi
highest = lax.Precision.HIGHEST


def tables(length, rows_index, cols_index):
    phase = rows_index[:, None] * cols_index[None, :] % length
    angle = phase.astype(jnp.float32) * (two_pi / length)
    return (jnp.cos(angle), jnp.sin(angle))


def reflect(values):
    return jnp.roll(jnp.flip(values, (1, 2)), (1, 1), axis=(1, 2))


def slab_plan(charges, green):
    gy_count = lax.axis_size("gy")
    gz_count = lax.axis_size("gz")
    groups = gy_count * gz_count
    half = NZ // 2
    per_device = half // groups
    col_block = charges.shape[1]
    depth = jnp.arange(NZ, dtype=jnp.int32)
    bins = jnp.arange(half, dtype=jnp.int32)
    indices = jnp.arange(NG, dtype=jnp.int32)
    cos_depth, sin_depth = tables(NZ, depth, bins)
    alternate = (1 - 2 * (depth % 2)).astype(jnp.float32)
    sin_packed = jnp.where(bins[None, :] == 0, -alternate[:, None], sin_depth)
    spec_re = jnp.einsum("xyz,zk->kxy", charges, cos_depth, precision=highest)
    spec_im = -jnp.einsum("xyz,zk->kxy", charges, sin_packed, precision=highest)
    own = jnp.moveaxis(green[:, :, :half], 2, 0)
    mirror = jnp.concatenate(
        [green[:, :, half : half + 1], jnp.flip(green[:, :, half + 1 :], 2)], axis=2
    )
    mirror = jnp.moveaxis(mirror, 2, 0)
    own, mirror = (
        lax.all_to_all(own, ("gy", "gz"), split_axis=0, concat_axis=2, tiled=True),
        lax.all_to_all(mirror, ("gy", "gz"), split_axis=0, concat_axis=2, tiled=True),
    )
    own, mirror = (
        lax.all_gather(own, "rep", axis=1, tiled=True),
        lax.all_gather(mirror, "rep", axis=1, tiled=True),
    )
    plane_re, plane_im = (
        lax.all_to_all(spec_re, ("gy", "gz"), split_axis=0, concat_axis=1, tiled=True),
        lax.all_to_all(spec_im, ("gy", "gz"), split_axis=0, concat_axis=1, tiled=True),
    )
    plane_re = plane_re.reshape(per_device, gy_count, NG, col_block)
    plane_im = plane_im.reshape(per_device, gy_count, NG, col_block)
    cos_plain, sin_plain = tables(NG, indices, indices)
    wide_cos = cos_plain.reshape(NG, gy_count, col_block)
    wide_sin = sin_plain.reshape(NG, gy_count, col_block)

    def second_in(matrix, values):
        return jnp.einsum("kgc,bgxc->bxk", matrix, values, precision=highest)

    def first_in(matrix, values):
        return jnp.einsum("kx,bxj->bkj", matrix, values, precision=highest)

    inner_re = second_in(wide_cos, plane_re) + second_in(wide_sin, plane_im)
    inner_im = second_in(wide_cos, plane_im) - second_in(wide_sin, plane_re)
    freq_re = first_in(cos_plain, inner_re) + first_in(sin_plain, inner_im)
    freq_im = first_in(cos_plain, inner_im) - first_in(sin_plain, inner_re)
    slot = lax.axis_index("gy") * gz_count + lax.axis_index("gz")
    packed = ((slot == 0) & (jnp.arange(per_device) == 0))[:, None, None]
    plain_gain = 0.5 * (own + reflect(mirror))
    first_gain = jnp.where(packed, 0.5 * (own + reflect(own)), plain_gain)
    second_gain = jnp.where(packed, 0.5 * (mirror + reflect(mirror)), plain_gain)
    mean_gain = 0.5 * (first_gain + second_gain)
    odd_gain = 0.5 * (first_gain - second_gain)
    prod_re = freq_re * mean_gain + reflect(freq_re) * odd_gain
    prod_im = freq_im * mean_gain - reflect(freq_im) * odd_gain
    undo_re = first_in(cos_plain, prod_re) - first_in(sin_plain, prod_im)
    undo_im = first_in(sin_plain, prod_re) + first_in(cos_plain, prod_im)

    def second_out(matrix, values):
        return jnp.einsum("kgc,bxk->bgxc", matrix, values, precision=highest)

    cells_re = second_out(wide_cos, undo_re) - second_out(wide_sin, undo_im)
    cells_im = second_out(wide_sin, undo_re) + second_out(wide_cos, undo_im)
    cells_re = cells_re.reshape(per_device, gy_count * NG, col_block)
    cells_im = cells_im.reshape(per_device, gy_count * NG, col_block)
    home_re, home_im = (
        lax.all_to_all(cells_re, ("gy", "gz"), split_axis=1, concat_axis=0, tiled=True),
        lax.all_to_all(cells_im, ("gy", "gz"), split_axis=1, concat_axis=0, tiled=True),
    )
    weight = jnp.where(bins == 0, 1.0, 2.0).astype(jnp.float32)
    cos_back = (cos_depth * weight[None, :]).T
    sin_back = jnp.where(bins[:, None] == 0, alternate[None, :], -2.0 * sin_depth.T)
    result_field = jnp.einsum("kxy,kz->xyz", home_re, cos_back, precision=highest)
    result_field = result_field + jnp.einsum("kxy,kz->xyz", home_im, sin_back, precision=highest)
    return result_field / (NG * NG * NZ)


f32 = jnp.float32
bf16 = jnp.bfloat16
MESH = pl.DeviceIdType.MESH
PARTS = 2
HALVES = 2


def split(values):
    high = values.astype(bf16)
    return high, (values - high.astype(f32)).astype(bf16)


def stacked_table(table, axis):
    rounded = table.astype(jnp.bfloat16)
    return jnp.asarray(np.stack([rounded, (table - rounded.astype(np.float64)).astype(jnp.bfloat16)], axis=axis))


def dot(left, right, dims=((1,), (0,))):
    return lax.dot_general(left, right, (dims, ((), ())), preferred_element_type=f32)


def dot_table(values, table_high, table_low, dims=((1,), (0,))):
    high, low = split(values)
    return dot(high, table_high, dims) + (dot(low, table_high, dims) + dot(high, table_low, dims))


def table_dot(table_high, table_low, values, dims=((1,), (0,))):
    high, low = split(values)
    return dot(table_high, high, dims) + (dot(table_high, low, dims) + dot(table_low, high, dims))


def depth_tables(length, groups, bins_each):
    per_part = bins_each // PARTS
    forward, back = [], []
    z = np.arange(length)
    alternate = 1.0 - 2.0 * (z % 2)
    for start in range(0, groups * bins_each, per_part):
        for imaginary in (False, True):
            for k in range(start, start + per_part):
                angle = 2.0 * np.pi * ((k * z) % length) / length
                if k == 0:
                    forward.append(alternate if imaginary else np.ones(length))
                    back.append(alternate if imaginary else np.ones(length))
                else:
                    forward.append(-np.sin(angle) if imaginary else np.cos(angle))
                    back.append(-2.0 * np.sin(angle) if imaginary else 2.0 * np.cos(angle))
    return np.stack(forward), np.stack(back)


def wide_table(table, axis):
    rounded = table.astype(jnp.bfloat16)
    low = (table - rounded.astype(np.float64)).astype(jnp.bfloat16)
    both = np.concatenate([rounded, rounded], axis=1 - axis)
    return jnp.asarray(np.concatenate([both, np.concatenate([low, np.zeros_like(low)], axis=1 - axis)], axis=axis))


def depth_in(table, cells, out):
    groups, parts, _, cols = out.shape
    rows, depth, step = cells.shape[0], cells.shape[2], 8

    def body(i, carry):
        values = jnp.concatenate(split(cells[pl.ds(i * step, step)].reshape(step * cols, depth)), axis=1)
        both = dot(table[...], values, ((1,), (1,)))
        result = both[:depth] + both[depth:]
        for row in range(step):
            piece = result[:, row * cols : (row + 1) * cols]
            at = pl.multiple_of(i * (step * 8) + row * 8, 8)
            out[:, :, pl.ds(at, 8), :] = piece.reshape(groups, parts, 8, cols)
        return carry

    lax.fori_loop(0, rows // step, body, 0)


def depth_out_kernel(table_ref, spec_ref, out_ref, held, sem):
    rows, cols, depth = out_ref.shape
    step = rows // sem.shape[0]
    copies = []
    for start in range(0, rows, step):
        pieces = [spec_ref[:, :, row * 8 : (row + 1) * 8, :].reshape(depth, cols) for row in range(start, start + step)]
        values = jnp.concatenate(split(jnp.concatenate(pieces, axis=1)), axis=0)
        both = dot(values, table_ref[...], ((0,), (0,)))
        at = pl.ds(start, step)
        held[at] = (both[:, :depth] + both[:, depth:]).reshape(step, cols, depth)
        copies.append(pltpu.make_async_copy(held.at[at], out_ref.at[at], sem.at[start // step]))
        copies[-1].start()
    for copy in copies:
        copy.wait()


def green_terms(count, green_ref):
    size, pitch, lanes = green_ref.shape
    flat = green_ref.reshape(size * pitch, lanes)
    rest = jnp.concatenate([flat[pl.ds(k2, size, stride=pitch), :] for k2 in range(count)], axis=0)
    return jnp.concatenate(split(rest), axis=1)


def pick_green(part, pick_ref, terms, out_ref):
    groups, parts, halves, rows, _ = out_ref.shape
    size = groups * halves * 8
    pick = pick_ref[part * 2 * size : (part + 1) * 2 * size, :]
    result = dot(jnp.concatenate([pick, pick], axis=1), terms, ((1,), (1,)))
    first_lanes = lax.broadcasted_iota(jnp.int32, (size, 128), 1) < 64
    place = lax.rem(lax.broadcasted_iota(jnp.int32, (size, 128), 0), 8) // 2
    for tile in range(rows // 8):
        spread = []
        for pair in (2 * tile, 2 * tile + 1):
            own = result[:size, pair * 128 : (pair + 1) * 128]
            mirror = result[size:, pair * 128 : (pair + 1) * 128]
            spread.append(jnp.where(first_lanes, own, pltpu.roll(mirror, 64, 1)))
            spread.append(jnp.where(first_lanes, pltpu.roll(own, 64, 1), mirror))
        packed = jnp.where(place < 2, jnp.where(place < 1, spread[0], spread[1]), jnp.where(place < 3, spread[2], spread[3]))
        out_ref[:, part, :, tile * 8 : (tile + 1) * 8, :] = packed.reshape(groups, halves, 8, 128)


def planes_kernel(
    gy_count, gz_count, reps,
    cells_in, green_in, pick_in, depth_table, waves_ref, flips_ref, home_ref,
    cells_ref, field_ref, pick_ref, depth_ref, gains_ref, spec_ref,
    planes, green, freq, tables, flips,
    fwd_send, fwd_recv, back_send, back_recv, green_send, green_recv, right_send, left_send, line_recv, own_sem, table_sem, in_sem,
):
    groups = gy_count * gz_count
    rep, gy, gz = lax.axis_index("rep"), lax.axis_index("gy"), lax.axis_index("gz")
    slot = gy * gz_count + gz
    rows = spec_ref.shape[2] // 8
    ng = flips_ref.shape[0]
    piece = gains_ref.shape[3]
    quarters = [(part, half) for part in range(PARTS) for half in range(HALVES)]

    def partner(step):
        there_y = lax.rem(gy + step // gz_count, gy_count)
        there_z = lax.rem(gz + step % gz_count, gz_count)
        return there_y * gz_count + there_z, {"rep": rep, "gy": there_y, "gz": there_z}

    def along(step):
        return {"rep": lax.rem(rep + step + reps, reps), "gy": gy, "gz": gz}

    inputs = [
        pltpu.make_async_copy(source, held, in_sem.at[i])
        for i, (source, held) in enumerate((
            (green_in, field_ref.at[:, pl.ds(0, green_in.shape[1]), :]), (pick_in, pick_ref), (cells_in, cells_ref), (depth_table, depth_ref)))
    ]
    for copy in inputs[:2]:
        copy.start()

    loads = []
    for table, swap in enumerate((False, True)):
        minus, plus = (1, 2) if swap else (2, 1)
        for quadrant, wave in enumerate((0, minus, plus, 0)):
            loads.append(pltpu.make_async_copy(
                waves_ref.at[wave],
                tables.at[table, :, pl.ds(quadrant // 2 * ng, ng), pl.ds(quadrant % 2 * ng, ng)],
                table_sem.at[4 * table + quadrant]))
    loads.append(pltpu.make_async_copy(flips_ref, flips, table_sem.at[8]))

    order = sorted(
        range(1, groups), key=lambda s: (s % gz_count == 0, s < gz_count, abs(s % gz_count - gz_count // 2), -s))

    barrier = pltpu.get_barrier_semaphore()
    for step in order:
        pl.semaphore_signal(barrier, inc=1, device_id=partner(step)[1], device_id_type=MESH)

    @pl.when(rep + 1 < reps)
    def _():
        pl.semaphore_signal(barrier, inc=1, device_id=along(1), device_id_type=MESH)

    @pl.when(rep >= 1)
    def _():
        pl.semaphore_signal(barrier, inc=1, device_id=along(-1), device_id_type=MESH)

    for copy in inputs[:2]:
        copy.wait()
    for copy in inputs[2:]:
        copy.start()
    terms = green_terms(green_in.shape[1], field_ref)
    pick_green(0, pick_ref, terms, gains_ref)
    pl.semaphore_wait(barrier, groups - 1 + lax.div(rep + reps - 1, reps) + lax.div(2 * reps - 2 - rep, reps))

    def green_copy(step, source, part, half):
        there, device = partner(step)
        return pltpu.make_async_remote_copy(
            src_ref=gains_ref.at[there, part, half], dst_ref=green.at[rep, part, half, pl.ds(source * piece, piece), :],
            send_sem=green_send.at[0], recv_sem=green_recv.at[part, half],
            device_id=device, device_id_type=MESH)

    def fwd_copy(step, source, part):
        there, device = partner(step)
        return pltpu.make_async_remote_copy(
            src_ref=spec_ref.at[there, part], dst_ref=planes.at[source, part],
            send_sem=fwd_send.at[0], recv_sem=fwd_recv.at[part], device_id=device, device_id_type=MESH)

    def back_copy(step, source, part):
        there, device = partner(step)
        return pltpu.make_async_remote_copy(
            src_ref=planes.at[there, part], dst_ref=home_ref.at[source, part],
            send_sem=back_send.at[0], recv_sem=back_recv.at[0], device_id=device, device_id_type=MESH)

    def whole(ref, sem):
        return pltpu.make_async_remote_copy(
            src_ref=ref, dst_ref=ref, send_sem=sem, recv_sem=sem, device_id=partner(1)[1], device_id_type=MESH)

    def line_copy(block, at, sem, step):
        return pltpu.make_async_remote_copy(
            src_ref=green.at[(block, *at)], dst_ref=green.at[(block, *at)], send_sem=sem,
            recv_sem=line_recv.at[(block, *at)], device_id=along(step), device_id_type=MESH)

    def green_start(part):
        for half in range(HALVES):
            for step in order:
                green_copy(step, slot, part, half).start()

    green_start(0)
    for part in range(1, PARTS):
        pick_green(part, pick_ref, terms, gains_ref)
        green_start(part)
    for part, half in quarters:
        green[rep, part, half, pl.ds(slot * piece, piece), :] = gains_ref[slot, part, half]
    for copy in inputs[2:]:
        copy.wait()
    for load in loads:
        load.start()
    depth_in(depth_ref, cells_ref, spec_ref)
    for part in range(PARTS):
        for step in order:
            fwd_copy(step, slot, part).start()
    planes[slot] = spec_ref[slot]
    others = pl.ds(0, groups - 1)

    def green_wait(at):
        whole(green.at[(rep, *at, pl.ds(0, (groups - 1) * piece))], green_recv.at[at]).wait_recv()

    def line_start(at, hop=None):
        right, left = rep + 1 < reps, rep >= 1
        if hop is not None:
            right, left = right & (rep == hop), left & (rep + hop == reps - 1)

        @pl.when(right)
        def _():
            line_copy(rep, at, right_send.at[0], 1).start()

        @pl.when(left)
        def _():
            line_copy(rep, at, left_send.at[0], -1).start()

    def relay(hop, at):
        @pl.when((rep >= hop) & (rep + 1 < reps))
        def _():
            line_copy(rep - hop, at, right_send.at[hop], 1).wait_recv()
            line_copy(rep - hop, at, right_send.at[hop], 1).start()

        @pl.when((rep + hop < reps) & (rep >= 1))
        def _():
            line_copy(rep + hop, at, left_send.at[hop], -1).wait_recv()
            line_copy(rep + hop, at, left_send.at[hop], -1).start()

    def line_end(at):
        for hop in range(1, reps):
            @pl.when(rep + 1 == reps)
            def _():
                line_copy(rep - hop, at, right_send.at[hop], 1).wait_recv()

            @pl.when(rep == 0)
            def _():
                line_copy(rep + hop, at, left_send.at[hop], -1).wait_recv()

    def load_plane(part, row):
        bands = []
        for y in range(gy_count):
            bands.append(jnp.concatenate(
                [planes[y * gz_count + x, part, pl.ds(row, rows, stride=8), :] for x in range(gz_count)], axis=0))
        return jnp.concatenate(bands, axis=1)

    def forward(part):
        def body(p, carry):
            values = jnp.concatenate([load_plane(part, p), load_plane(part, 4 + p)], axis=1)
            inner = dot_table(values, tables[0, 0], tables[0, 1])
            inner = jnp.concatenate([inner[:, :ng], inner[:, ng:]], axis=0)
            freq[part * 4 + p] = table_dot(tables[1, 0], tables[1, 1], inner)
            return carry

        lax.fori_loop(0, 4, body, 0)

    def reflect_plane(values):
        high, low = split(values)
        turned = dot(flips[...], high) + dot(flips[...], low)
        high, low = split(turned)
        return dot(high, flips[...]) + dot(low, flips[...])

    def backward(part, half):
        def body(p, carry):
            row = half * 2 + p
            plane = part * 4 + row
            own, mirror = [], []
            lane = lax.broadcasted_iota(jnp.int32, (ng, 128), 1)
            for r in range(0, reps, 2):
                one, two = (green[q, part, half, pl.ds(p, ng, stride=2), :] for q in (r, r + 1))
                own.append(jnp.where(lane < 64, one, pltpu.roll(two, 64, 1)))
                mirror.append(jnp.where(lane < 64, pltpu.roll(one, 64, 1), two))
            own = jnp.concatenate(own, axis=1).T
            mirror = jnp.concatenate(mirror, axis=1).T
            packed = (slot == 0) & (plane == 0)

            @pl.when(jnp.logical_not(packed))
            def _():
                gain = 0.5 * (own + reflect_plane(mirror))
                freq[plane] = freq[plane] * jnp.concatenate([gain, gain], axis=0)

            @pl.when(packed)
            def _():
                first = 0.5 * (own + reflect_plane(own))
                second = 0.5 * (mirror + reflect_plane(mirror))
                mean, odd = 0.5 * (first + second), 0.5 * (first - second)
                real, imag = freq[plane, :ng, :], freq[plane, ng:, :]
                freq[plane, :ng, :] = real * mean + reflect_plane(real) * odd
                freq[plane, ng:, :] = imag * mean - reflect_plane(imag) * odd

            undo = table_dot(tables[0, 0], tables[0, 1], freq[plane])
            undo = jnp.concatenate([undo[:ng], undo[ng:]], axis=1)
            cells = dot_table(undo, tables[1, 0], tables[1, 1])
            cols = ng // gy_count
            for c in range(2):
                for y in range(gy_count):
                    for x in range(gz_count):
                        planes[y * gz_count + x, part, pl.ds(c * 4 + row, rows, stride=8), :] = cells[
                            x * rows : (x + 1) * rows, c * ng + y * cols : c * ng + (y + 1) * cols]
            return carry

        lax.fori_loop(0, 2, body, 0)

    own_home = [pltpu.make_async_copy(planes.at[slot, h], home_ref.at[slot, h], own_sem.at[h]) for h in range(PARTS)]

    def arrive(part):
        whole(planes.at[others, part], fwd_recv.at[part]).wait_recv()
        forward(part)

    def depart(part):
        for step in order:
            back_copy(step, slot, part).start()
        own_home[part].start()

    first, second = quarters[:HALVES], quarters[HALVES:]

    def second_start(hop):
        for at in second:
            line_start(at, hop)

    for at in first:
        green_wait(at)
        line_start(at)
    relay(1, first[0])
    for at in second:
        green_wait(at)
    second_start(0)
    relay(1, first[1])
    second_start(1)
    for hop in range(2, reps - 1):
        for at in first:
            relay(hop, at)
        second_start(hop)
    for load in loads:
        load.wait()
    relay(1, second[0])
    arrive(0)
    relay(1, second[1])
    for at in first:
        line_end(at)
        backward(*at)
        if at == first[-1]:
            depart(0)
        for hop in range(2, reps - 1):
            relay(hop, second[at[1]])
    arrive(1)
    for at in second:
        line_end(at)
        backward(*at)
    depart(1)

    whole(gains_ref.at[others], green_send.at[0]).wait_send()
    whole(spec_ref.at[others], fwd_send.at[0]).wait_send()
    for hop in range(reps):
        @pl.when((rep >= hop) & (rep + 1 < reps))
        def _():
            whole(green.at[rep - hop], right_send.at[hop]).wait_send()

        @pl.when((rep + hop < reps) & (rep >= 1))
        def _():
            whole(green.at[rep + hop], left_send.at[hop]).wait_send()
    for part in range(PARTS):
        own_home[part].wait()
    whole(planes.at[others], back_send.at[0]).wait_send()
    whole(home_ref.at[others], back_recv.at[0]).wait_recv()


def fused_plan(charges, green):
    gy_count, gz_count, reps = lax.axis_size("gy"), lax.axis_size("gz"), lax.axis_size("rep")
    groups = gy_count * gz_count
    rows, cols, depth = charges.shape
    ng = rows * gz_count
    half = depth // 2
    each = half // groups
    forward_table, back_table = depth_tables(depth, groups, each)
    chunks = rows // 8
    spec_shape = jax.ShapeDtypeStruct((groups, PARTS, rows * 8, cols), f32)

    k1, k2, _ = green.shape
    own_index = np.arange(half)
    opposite = np.where(own_index == 0, half, depth - own_index)
    quad, place = np.divmod(np.arange(groups * HALVES * 8), 8)
    quad = quad // HALVES * PARTS * HALVES + quad % HALVES
    pick = []
    for part in range(PARTS):
        bins = (quad + part * HALVES) * 2 + place % 2
        pick += [own_index[bins], opposite[bins]]
    pick = (np.concatenate(pick)[:, None] == np.arange(depth)[None, :]).astype(np.float32)
    index = np.arange(ng)
    angle = 2.0 * np.pi * ((index[:, None] * index[None, :]) % ng) / ng
    cos, sin = np.cos(angle), np.sin(angle)
    waves = stacked_table(np.stack([cos, sin, -sin]), 1)
    flips = jnp.asarray((index[:, None] + index[None, :]) % ng == 0, bf16)

    dma = pltpu.SemaphoreType.DMA
    home = pl.pallas_call(
        functools.partial(planes_kernel, gy_count, gz_count, reps),
        out_shape=spec_shape, name="planes",
        in_specs=[pl.BlockSpec(memory_space=pl.ANY)] * 6, out_specs=pl.BlockSpec(memory_space=pl.ANY),
        scratch_shapes=[
            pltpu.VMEM(charges.shape, f32),
            pltpu.VMEM((k1, k2 + 8, depth), f32),
            pltpu.VMEM(pick.shape, bf16),
            pltpu.VMEM((2 * depth, 2 * depth), bf16),
            pltpu.VMEM((groups, PARTS, HALVES, k2 * 2, 2 * k1), f32),
            pltpu.VMEM(spec_shape.shape, f32),
            pltpu.VMEM(spec_shape.shape, f32),
            pltpu.VMEM((reps, PARTS, HALVES, ng * 2, 2 * k1), f32),
            pltpu.VMEM((each, 2 * ng, ng), f32),
            pltpu.VMEM((2, 2, 2 * ng, 2 * ng), bf16),
            pltpu.VMEM((ng, ng), bf16),
            dma((1,)), dma((PARTS,)), dma((1,)), dma((1,)), dma((1,)), dma((PARTS, HALVES)),
            dma((reps,)), dma((reps,)), dma((reps, PARTS, HALVES)), dma((PARTS,)), dma((9,)), dma((4,)),
        ],
        compiler_params=pltpu.CompilerParams(
            collective_id=0, has_side_effects=True, vmem_limit_bytes=44 * 2**20),
    )(*(
        pltpu.with_memory_space_constraint(value, pltpu.HBM)
        for value in (
            charges, green, jnp.asarray(pick, bf16), wide_table(forward_table, 0), waves, flips)
    ))

    vmem = pl.BlockSpec(memory_space=pltpu.VMEM)
    return pl.pallas_call(
        depth_out_kernel, out_shape=jax.ShapeDtypeStruct(charges.shape, f32), name="depth_out",
        in_specs=[vmem, vmem], out_specs=pl.BlockSpec(memory_space=pl.ANY),
        scratch_shapes=[pltpu.VMEM(charges.shape, f32), dma((chunks,))],
        compiler_params=pltpu.CompilerParams(vmem_limit_bytes=16 * 2**20),
    )(wide_table(back_table / (ng * ng * depth), 1), home)


def on_device(charges, green):
    groups = lax.axis_size("gy") * lax.axis_size("gz")
    rows, cols, depth = charges.shape
    aligned = (
        cols % 128 == 0 and depth % 128 == 0 and depth == 16 * groups and rows % 8 == 0
        and green.shape[0] == 64 and lax.axis_size("rep") % 2 == 0 and lax.axis_size("rep") > 2
        and rows * lax.axis_size("gz") == cols * lax.axis_size("gy")
    )
    return fused_plan(charges, green) if aligned else slab_plan(charges, green)


def solution(mesh):
    placed = (P(("rep", "gz"), "gy", None), P("rep", ("gy", "gz"), None))
    return jax.shard_map(
        on_device,
        mesh=mesh,
        in_specs=placed,
        out_specs=P(("rep", "gz"), "gy", None),
        check_vma=False,
    )
```

```python
import functools
import math

import jax
import jax.numpy as jnp
import numpy as np
from jax import lax
from jax.experimental import pallas as pl
from jax.experimental.pallas import tpu as pltpu
from jax.sharding import PartitionSpec as P

NG = 256
NZ = 128


two_pi = 2.0 * math.pi
highest = lax.Precision.HIGHEST


def tables(length, rows_index, cols_index):
    phase = rows_index[:, None] * cols_index[None, :] % length
    angle = phase.astype(jnp.float32) * (two_pi / length)
    return (jnp.cos(angle), jnp.sin(angle))


def reflect(values):
    return jnp.roll(jnp.flip(values, (1, 2)), (1, 1), axis=(1, 2))


def slab_plan(charges, green):
    gy_count = lax.axis_size("gy")
    gz_count = lax.axis_size("gz")
    groups = gy_count * gz_count
    half = NZ // 2
    per_device = half // groups
    col_block = charges.shape[1]
    depth = jnp.arange(NZ, dtype=jnp.int32)
    bins = jnp.arange(half, dtype=jnp.int32)
    indices = jnp.arange(NG, dtype=jnp.int32)
    cos_depth, sin_depth = tables(NZ, depth, bins)
    alternate = (1 - 2 * (depth % 2)).astype(jnp.float32)
    sin_packed = jnp.where(bins[None, :] == 0, -alternate[:, None], sin_depth)
    spec_re = jnp.einsum("xyz,zk->kxy", charges, cos_depth, precision=highest)
    spec_im = -jnp.einsum("xyz,zk->kxy", charges, sin_packed, precision=highest)
    own = jnp.moveaxis(green[:, :, :half], 2, 0)
    mirror = jnp.concatenate(
        [green[:, :, half : half + 1], jnp.flip(green[:, :, half + 1 :], 2)], axis=2
    )
    mirror = jnp.moveaxis(mirror, 2, 0)
    own, mirror = (
        lax.all_to_all(own, ("gy", "gz"), split_axis=0, concat_axis=2, tiled=True),
        lax.all_to_all(mirror, ("gy", "gz"), split_axis=0, concat_axis=2, tiled=True),
    )
    own, mirror = (
        lax.all_gather(own, "rep", axis=1, tiled=True),
        lax.all_gather(mirror, "rep", axis=1, tiled=True),
    )
    plane_re, plane_im = (
        lax.all_to_all(spec_re, ("gy", "gz"), split_axis=0, concat_axis=1, tiled=True),
        lax.all_to_all(spec_im, ("gy", "gz"), split_axis=0, concat_axis=1, tiled=True),
    )
    plane_re = plane_re.reshape(per_device, gy_count, NG, col_block)
    plane_im = plane_im.reshape(per_device, gy_count, NG, col_block)
    cos_plain, sin_plain = tables(NG, indices, indices)
    wide_cos = cos_plain.reshape(NG, gy_count, col_block)
    wide_sin = sin_plain.reshape(NG, gy_count, col_block)

    def second_in(matrix, values):
        return jnp.einsum("kgc,bgxc->bxk", matrix, values, precision=highest)

    def first_in(matrix, values):
        return jnp.einsum("kx,bxj->bkj", matrix, values, precision=highest)

    inner_re = second_in(wide_cos, plane_re) + second_in(wide_sin, plane_im)
    inner_im = second_in(wide_cos, plane_im) - second_in(wide_sin, plane_re)
    freq_re = first_in(cos_plain, inner_re) + first_in(sin_plain, inner_im)
    freq_im = first_in(cos_plain, inner_im) - first_in(sin_plain, inner_re)
    slot = lax.axis_index("gy") * gz_count + lax.axis_index("gz")
    packed = ((slot == 0) & (jnp.arange(per_device) == 0))[:, None, None]
    plain_gain = 0.5 * (own + reflect(mirror))
    first_gain = jnp.where(packed, 0.5 * (own + reflect(own)), plain_gain)
    second_gain = jnp.where(packed, 0.5 * (mirror + reflect(mirror)), plain_gain)
    mean_gain = 0.5 * (first_gain + second_gain)
    odd_gain = 0.5 * (first_gain - second_gain)
    prod_re = freq_re * mean_gain + reflect(freq_re) * odd_gain
    prod_im = freq_im * mean_gain - reflect(freq_im) * odd_gain
    undo_re = first_in(cos_plain, prod_re) - first_in(sin_plain, prod_im)
    undo_im = first_in(sin_plain, prod_re) + first_in(cos_plain, prod_im)

    def second_out(matrix, values):
        return jnp.einsum("kgc,bxk->bgxc", matrix, values, precision=highest)

    cells_re = second_out(wide_cos, undo_re) - second_out(wide_sin, undo_im)
    cells_im = second_out(wide_sin, undo_re) + second_out(wide_cos, undo_im)
    cells_re = cells_re.reshape(per_device, gy_count * NG, col_block)
    cells_im = cells_im.reshape(per_device, gy_count * NG, col_block)
    home_re, home_im = (
        lax.all_to_all(cells_re, ("gy", "gz"), split_axis=1, concat_axis=0, tiled=True),
        lax.all_to_all(cells_im, ("gy", "gz"), split_axis=1, concat_axis=0, tiled=True),
    )
    weight = jnp.where(bins == 0, 1.0, 2.0).astype(jnp.float32)
    cos_back = (cos_depth * weight[None, :]).T
    sin_back = jnp.where(bins[:, None] == 0, alternate[None, :], -2.0 * sin_depth.T)
    result_field = jnp.einsum("kxy,kz->xyz", home_re, cos_back, precision=highest)
    result_field = result_field + jnp.einsum("kxy,kz->xyz", home_im, sin_back, precision=highest)
    return result_field / (NG * NG * NZ)


f32 = jnp.float32
bf16 = jnp.bfloat16
MESH = pl.DeviceIdType.MESH
PARTS = 2
HALVES = 2


def split(values):
    high = values.astype(bf16)
    return high, (values - high.astype(f32)).astype(bf16)


def stacked_table(table, axis):
    rounded = table.astype(jnp.bfloat16)
    return jnp.asarray(np.stack([rounded, (table - rounded.astype(np.float64)).astype(jnp.bfloat16)], axis=axis))


def dot(left, right, dims=((1,), (0,))):
    return lax.dot_general(left, right, (dims, ((), ())), preferred_element_type=f32)


def dot_table(values, table_high, table_low, dims=((1,), (0,))):
    high, low = split(values)
    return dot(high, table_high, dims) + (dot(low, table_high, dims) + dot(high, table_low, dims))


def table_dot(table_high, table_low, values, dims=((1,), (0,))):
    high, low = split(values)
    return dot(table_high, high, dims) + (dot(table_high, low, dims) + dot(table_low, high, dims))


def depth_tables(length, groups, bins_each):
    per_part = bins_each // PARTS
    forward, back = [], []
    z = np.arange(length)
    alternate = 1.0 - 2.0 * (z % 2)
    for start in range(0, groups * bins_each, per_part):
        for imaginary in (False, True):
            for k in range(start, start + per_part):
                angle = 2.0 * np.pi * ((k * z) % length) / length
                if k == 0:
                    forward.append(alternate if imaginary else np.ones(length))
                    back.append(alternate if imaginary else np.ones(length))
                else:
                    forward.append(-np.sin(angle) if imaginary else np.cos(angle))
                    back.append(-2.0 * np.sin(angle) if imaginary else 2.0 * np.cos(angle))
    return np.stack(forward), np.stack(back)


def wide_table(table, axis):
    rounded = table.astype(jnp.bfloat16)
    low = (table - rounded.astype(np.float64)).astype(jnp.bfloat16)
    both = np.concatenate([rounded, rounded], axis=1 - axis)
    return jnp.asarray(np.concatenate([both, np.concatenate([low, np.zeros_like(low)], axis=1 - axis)], axis=axis))


def depth_in(table, cells, out):
    groups, parts, _, cols = out.shape
    rows, depth, step = cells.shape[0], cells.shape[2], 8

    def body(i, carry):
        values = jnp.concatenate(split(cells[pl.ds(i * step, step)].reshape(step * cols, depth)), axis=1)
        both = dot(table[...], values, ((1,), (1,)))
        result = both[:depth] + both[depth:]
        for row in range(step):
            piece = result[:, row * cols : (row + 1) * cols]
            at = pl.multiple_of(i * (step * 8) + row * 8, 8)
            out[:, :, pl.ds(at, 8), :] = piece.reshape(groups, parts, 8, cols)
        return carry

    lax.fori_loop(0, rows // step, body, 0)


def depth_out_kernel(table_ref, spec_ref, out_ref, held, sem):
    rows, cols, depth = out_ref.shape
    step = rows // sem.shape[0]
    copies = []
    for start in range(0, rows, step):
        pieces = [spec_ref[:, :, row * 8 : (row + 1) * 8, :].reshape(depth, cols) for row in range(start, start + step)]
        values = jnp.concatenate(split(jnp.concatenate(pieces, axis=1)), axis=0)
        both = dot(values, table_ref[...], ((0,), (0,)))
        at = pl.ds(start, step)
        held[at] = (both[:, :depth] + both[:, depth:]).reshape(step, cols, depth)
        copies.append(pltpu.make_async_copy(held.at[at], out_ref.at[at], sem.at[start // step]))
        copies[-1].start()
    for copy in copies:
        copy.wait()


def green_terms(count, green_ref):
    size, pitch, lanes = green_ref.shape
    flat = green_ref.reshape(size * pitch, lanes)
    rest = jnp.concatenate([flat[pl.ds(k2, size, stride=pitch), :] for k2 in range(count)], axis=0)
    return jnp.concatenate(split(rest), axis=1)


def pick_green(part, pick_ref, terms, out_ref):
    groups, parts, halves, rows, _ = out_ref.shape
    size = groups * halves * 8
    pick = pick_ref[part * 2 * size : (part + 1) * 2 * size, :]
    result = dot(jnp.concatenate([pick, pick], axis=1), terms, ((1,), (1,)))
    first_lanes = lax.broadcasted_iota(jnp.int32, (size, 128), 1) < 64
    place = lax.rem(lax.broadcasted_iota(jnp.int32, (size, 128), 0), 8) // 2
    even = (place == 0) | (place == 2)
    stays = first_lanes == even
    for tile in range(rows // 8):
        own, mirror = (
            jnp.where(
                place < 2, result[start : start + size, tile * 256 : tile * 256 + 128],
                result[start : start + size, tile * 256 + 128 : (tile + 1) * 256])
            for start in (0, size)
        )
        packed = jnp.where(
            stays, jnp.where(even, own, mirror), pltpu.roll(jnp.where(even, mirror, own), 64, 1))
        out_ref[:, part, :, tile * 8 : (tile + 1) * 8, :] = packed.reshape(groups, halves, 8, 128)


def planes_kernel(
    gy_count, gz_count, reps,
    cells_in, green_in, pick_in, depth_table, waves_ref, flips_ref, home_ref,
    cells_ref, field_ref, pick_ref, depth_ref, gains_ref, spec_ref,
    planes, green, freq, waves, tables, flips,
    fwd_send, fwd_recv, back_send, back_recv, green_send, green_recv, right_send, left_send, line_recv, own_sem, table_sem, in_sem,
):
    groups = gy_count * gz_count
    rep, gy, gz = lax.axis_index("rep"), lax.axis_index("gy"), lax.axis_index("gz")
    slot = gy * gz_count + gz
    rows = spec_ref.shape[2] // 8
    ng = flips_ref.shape[0]
    piece = gains_ref.shape[3]
    quarters = [(part, half) for part in range(PARTS) for half in range(HALVES)]

    def partner(step):
        there_y = lax.rem(gy + step // gz_count, gy_count)
        there_z = lax.rem(gz + step % gz_count, gz_count)
        return there_y * gz_count + there_z, {"rep": rep, "gy": there_y, "gz": there_z}

    def along(step):
        return {"rep": lax.rem(rep + step + reps, reps), "gy": gy, "gz": gz}

    inputs = [
        pltpu.make_async_copy(source, held, in_sem.at[i])
        for i, (source, held) in enumerate((
            (green_in, field_ref.at[:, pl.ds(0, green_in.shape[1]), :]), (pick_in, pick_ref), (cells_in, cells_ref), (depth_table, depth_ref)))
    ]
    for copy in inputs[:2]:
        copy.start()

    loads = [
        pltpu.make_async_copy(source, held, table_sem.at[i])
        for i, (source, held) in enumerate(((waves_ref, waves), (flips_ref, flips)))
    ]

    order = sorted(
        range(1, groups), key=lambda s: (s % gz_count == 0, s < gz_count, abs(s % gz_count - gz_count // 2), -s))

    barrier = pltpu.get_barrier_semaphore()
    for step in order:
        pl.semaphore_signal(barrier, inc=1, device_id=partner(step)[1], device_id_type=MESH)

    @pl.when(rep + 1 < reps)
    def _():
        pl.semaphore_signal(barrier, inc=1, device_id=along(1), device_id_type=MESH)

    @pl.when(rep >= 1)
    def _():
        pl.semaphore_signal(barrier, inc=1, device_id=along(-1), device_id_type=MESH)

    for copy in inputs[:2]:
        copy.wait()
    for copy in inputs[2:]:
        copy.start()
    terms = green_terms(green_in.shape[1], field_ref)
    pick_green(0, pick_ref, terms, gains_ref)
    pl.semaphore_wait(barrier, groups - 1 + lax.div(rep + reps - 1, reps) + lax.div(2 * reps - 2 - rep, reps))

    def green_copy(step, source, part, half):
        there, device = partner(step)
        return pltpu.make_async_remote_copy(
            src_ref=gains_ref.at[there, part, half], dst_ref=green.at[rep, part, half, pl.ds(source * piece, piece), :],
            send_sem=green_send.at[0], recv_sem=green_recv.at[part, half],
            device_id=device, device_id_type=MESH)

    def fwd_copy(step, source, part):
        there, device = partner(step)
        return pltpu.make_async_remote_copy(
            src_ref=spec_ref.at[there, part], dst_ref=planes.at[source, part],
            send_sem=fwd_send.at[0], recv_sem=fwd_recv.at[part], device_id=device, device_id_type=MESH)

    def back_copy(step, source, part):
        there, device = partner(step)
        return pltpu.make_async_remote_copy(
            src_ref=planes.at[there, part], dst_ref=home_ref.at[source, part],
            send_sem=back_send.at[0], recv_sem=back_recv.at[0], device_id=device, device_id_type=MESH)

    def whole(ref, sem):
        return pltpu.make_async_remote_copy(
            src_ref=ref, dst_ref=ref, send_sem=sem, recv_sem=sem, device_id=partner(1)[1], device_id_type=MESH)

    def line_copy(block, at, sem, step):
        return pltpu.make_async_remote_copy(
            src_ref=green.at[(block, *at)], dst_ref=green.at[(block, *at)], send_sem=sem,
            recv_sem=line_recv.at[(block, *at)], device_id=along(step), device_id_type=MESH)

    def green_start(part):
        for half in range(HALVES):
            for step in order:
                green_copy(step, slot, part, half).start()

    green_start(0)
    for part in range(1, PARTS):
        pick_green(part, pick_ref, terms, gains_ref)
        green_start(part)
    for part, half in quarters:
        green[rep, part, half, pl.ds(slot * piece, piece), :] = gains_ref[slot, part, half]
    for copy in inputs[2:]:
        copy.wait()
    for load in loads:
        load.start()
    depth_in(depth_ref, cells_ref, spec_ref)
    for part in range(PARTS):
        for step in order:
            fwd_copy(step, slot, part).start()
    planes[slot] = spec_ref[slot]
    others = pl.ds(0, groups - 1)

    def green_wait(at):
        whole(green.at[(rep, *at, pl.ds(0, (groups - 1) * piece))], green_recv.at[at]).wait_recv()

    def line_start(at, hop=None):
        right, left = rep + 1 < reps, rep >= 1
        if hop is not None:
            right, left = right & (rep == hop), left & (rep + hop == reps - 1)

        @pl.when(right)
        def _():
            line_copy(rep, at, right_send.at[0], 1).start()

        @pl.when(left)
        def _():
            line_copy(rep, at, left_send.at[0], -1).start()

    def relay(hop, at):
        @pl.when((rep >= hop) & (rep + 1 < reps))
        def _():
            line_copy(rep - hop, at, right_send.at[0], 1).wait_recv()
            line_copy(rep - hop, at, right_send.at[0], 1).start()

        @pl.when((rep + hop < reps) & (rep >= 1))
        def _():
            line_copy(rep + hop, at, left_send.at[0], -1).wait_recv()
            line_copy(rep + hop, at, left_send.at[0], -1).start()

    def line_end(at):
        for hop in range(1, reps):
            @pl.when(rep + 1 == reps)
            def _():
                line_copy(rep - hop, at, right_send.at[0], 1).wait_recv()

            @pl.when(rep == 0)
            def _():
                line_copy(rep + hop, at, left_send.at[0], -1).wait_recv()

    def load_plane(part, row):
        bands = []
        for y in range(gy_count):
            bands.append(jnp.concatenate(
                [planes[y * gz_count + x, part, pl.ds(row, rows, stride=8), :] for x in range(gz_count)], axis=0))
        return jnp.concatenate(bands, axis=1)

    def forward(part):
        def body(p, carry):
            values = jnp.concatenate([load_plane(part, p), load_plane(part, 4 + p)], axis=1)
            inner = dot_table(values, tables[0, 0], tables[0, 1])
            inner = jnp.concatenate([inner[:, :ng], inner[:, ng:]], axis=0)
            freq[part * 4 + p] = table_dot(tables[1, 0], tables[1, 1], inner)
            return carry

        lax.fori_loop(0, 4, body, 0)

    def reflect_plane(values):
        high, low = split(values)
        turned = dot(flips[...], high) + dot(flips[...], low)
        high, low = split(turned)
        return dot(high, flips[...]) + dot(low, flips[...])

    def backward(part, half):
        def body(p):
            row = half * 2 + p
            plane = part * 4 + row
            own, mirror = [], []
            lane = lax.broadcasted_iota(jnp.int32, (ng, 128), 1)
            for r in range(0, reps, 2):
                one, two = (green[q, part, half, pl.ds(p, ng, stride=2), :] for q in (r, r + 1))
                own.append(jnp.where(lane < 64, one, pltpu.roll(two, 64, 1)))
                mirror.append(jnp.where(lane < 64, pltpu.roll(one, 64, 1), two))
            own = jnp.concatenate(own, axis=1).T
            mirror = jnp.concatenate(mirror, axis=1).T

            def plain():
                gain = 0.5 * (own + reflect_plane(mirror))
                freq[plane] = freq[plane] * jnp.concatenate([gain, gain], axis=0)

            if plane == 0:
                packed = slot == 0

                @pl.when(jnp.logical_not(packed))
                def _():
                    plain()

                @pl.when(packed)
                def _():
                    first = 0.5 * (own + reflect_plane(own))
                    second = 0.5 * (mirror + reflect_plane(mirror))
                    mean, odd = 0.5 * (first + second), 0.5 * (first - second)
                    real, imag = freq[plane, :ng, :], freq[plane, ng:, :]
                    freq[plane, :ng, :] = real * mean + reflect_plane(real) * odd
                    freq[plane, ng:, :] = imag * mean - reflect_plane(imag) * odd
            else:
                plain()

            undo = table_dot(tables[0, 0], tables[0, 1], freq[plane])
            undo = jnp.concatenate([undo[:ng], undo[ng:]], axis=1)
            cells = dot_table(undo, tables[1, 0], tables[1, 1])
            cols = ng // gy_count
            for c in range(2):
                for y in range(gy_count):
                    for x in range(gz_count):
                        planes[y * gz_count + x, part, pl.ds(c * 4 + row, rows, stride=8), :] = cells[
                            x * rows : (x + 1) * rows, c * ng + y * cols : c * ng + (y + 1) * cols]

        for p in range(2):
            body(p)

    own_home = [pltpu.make_async_copy(planes.at[slot, h], home_ref.at[slot, h], own_sem.at[0]) for h in range(PARTS)]

    def arrive(part):
        whole(planes.at[others, part], fwd_recv.at[part]).wait_recv()
        forward(part)

    def depart(part):
        for step in order:
            back_copy(step, slot, part).start()
        own_home[part].start()

    first, second = quarters[:HALVES], quarters[HALVES:]

    def second_relay(hop):
        relay(hop, second[0])
        line_start(second[1], hop)

    for at in first:
        green_wait(at)
        line_start(at)
    relay(1, first[0])
    for at in second:
        green_wait(at)
    for at in second:
        line_start(at, 0)
    relay(1, first[1])
    line_start(second[0], 1)
    for hop in range(2, reps - 1):
        for at in first:
            relay(hop, at)
        line_start(second[0], hop)
    for load in loads:
        load.wait()
    for table, swap in enumerate((False, True)):
        minus, plus = (1, 2) if swap else (2, 1)
        for quadrant, wave in enumerate((0, minus, plus, 0)):
            down, right = quadrant // 2 * ng, quadrant % 2 * ng
            tables[table, :, down : down + ng, right : right + ng] = waves[wave]
    second_relay(1)
    arrive(0)
    for at in first:
        line_end(at)
        backward(*at)
        if at == first[0]:
            for hop in range(2, reps - 1):
                second_relay(hop)
    depart(0)
    for hop in range(1, reps - 1):
        relay(hop, second[1])
    arrive(1)
    for at in second:
        line_end(at)
        backward(*at)
    depart(1)

    whole(gains_ref.at[others], green_send.at[0]).wait_send()
    whole(spec_ref.at[others], fwd_send.at[0]).wait_send()
    for at in range(1, reps):
        @pl.when(rep + 1 == at)
        def _():
            whole(green.at[pl.ds(0, at)], right_send.at[0]).wait_send()

        @pl.when(rep == at)
        def _():
            whole(green.at[pl.ds(at, reps - at)], left_send.at[0]).wait_send()
    pltpu.make_async_copy(planes.at[slot], home_ref.at[slot], own_sem.at[0]).wait()
    whole(planes.at[others], back_send.at[0]).wait_send()
    whole(home_ref.at[others], back_recv.at[0]).wait_recv()


def fused_plan(charges, green):
    gy_count, gz_count, reps = lax.axis_size("gy"), lax.axis_size("gz"), lax.axis_size("rep")
    groups = gy_count * gz_count
    rows, cols, depth = charges.shape
    ng = rows * gz_count
    half = depth // 2
    each = half // groups
    forward_table, back_table = depth_tables(depth, groups, each)
    chunks = rows // 8
    spec_shape = jax.ShapeDtypeStruct((groups, PARTS, rows * 8, cols), f32)

    k1, k2, _ = green.shape
    own_index = np.arange(half)
    opposite = np.where(own_index == 0, half, depth - own_index)
    quad, place = np.divmod(np.arange(groups * HALVES * 8), 8)
    quad = quad // HALVES * PARTS * HALVES + quad % HALVES
    pick = []
    for part in range(PARTS):
        bins = (quad + part * HALVES) * 2 + place % 2
        pick += [own_index[bins], opposite[bins]]
    pick = (np.concatenate(pick)[:, None] == np.arange(depth)[None, :]).astype(np.float32)
    index = np.arange(ng)
    angle = 2.0 * np.pi * ((index[:, None] * index[None, :]) % ng) / ng
    cos, sin = np.cos(angle), np.sin(angle)
    waves = stacked_table(np.stack([cos, sin, -sin]), 1)
    flips = jnp.asarray((index[:, None] + index[None, :]) % ng == 0, bf16)

    dma = pltpu.SemaphoreType.DMA
    home = pl.pallas_call(
        functools.partial(planes_kernel, gy_count, gz_count, reps),
        out_shape=spec_shape, name="planes",
        in_specs=[pl.BlockSpec(memory_space=pl.ANY)] * 6, out_specs=pl.BlockSpec(memory_space=pl.ANY),
        scratch_shapes=[
            pltpu.VMEM(charges.shape, f32),
            pltpu.VMEM((k1, k2 + 8, depth), f32),
            pltpu.VMEM(pick.shape, bf16),
            pltpu.VMEM((2 * depth, 2 * depth), bf16),
            pltpu.VMEM((groups, PARTS, HALVES, k2 * 2, 2 * k1), f32),
            pltpu.VMEM(spec_shape.shape, f32),
            pltpu.VMEM(spec_shape.shape, f32),
            pltpu.VMEM((reps, PARTS, HALVES, ng * 2, 2 * k1), f32),
            pltpu.VMEM((each, 2 * ng, ng), f32),
            pltpu.VMEM(waves.shape, bf16),
            pltpu.VMEM((2, 2, 2 * ng, 2 * ng), bf16),
            pltpu.VMEM((ng, ng), bf16),
            dma((1,)), dma((PARTS,)), dma((1,)), dma((1,)), dma((1,)), dma((PARTS, HALVES)),
            dma((1,)), dma((1,)), dma((reps, PARTS, HALVES)), dma((1,)), dma((2,)), dma((4,)),
        ],
        compiler_params=pltpu.CompilerParams(
            collective_id=0, has_side_effects=True, vmem_limit_bytes=44 * 2**20),
    )(*(
        pltpu.with_memory_space_constraint(value, pltpu.HBM)
        for value in (
            charges, green, jnp.asarray(pick, bf16), wide_table(forward_table, 0), waves, flips)
    ))

    vmem = pl.BlockSpec(memory_space=pltpu.VMEM)
    return pl.pallas_call(
        depth_out_kernel, out_shape=jax.ShapeDtypeStruct(charges.shape, f32), name="depth_out",
        in_specs=[vmem, vmem], out_specs=pl.BlockSpec(memory_space=pl.ANY),
        scratch_shapes=[pltpu.VMEM(charges.shape, f32), dma((chunks,))],
        compiler_params=pltpu.CompilerParams(vmem_limit_bytes=16 * 2**20),
    )(wide_table(back_table / (ng * ng * depth), 1), home)


def on_device(charges, green):
    groups = lax.axis_size("gy") * lax.axis_size("gz")
    rows, cols, depth = charges.shape
    aligned = (
        cols % 128 == 0 and depth % 128 == 0 and depth == 16 * groups and rows % 8 == 0
        and green.shape[0] == 64 and lax.axis_size("rep") % 2 == 0 and lax.axis_size("rep") > 2
        and rows * lax.axis_size("gz") == cols * lax.axis_size("gy")
    )
    return fused_plan(charges, green) if aligned else slab_plan(charges, green)


def solution(mesh):
    placed = (P(("rep", "gz"), "gy", None), P("rep", ("gy", "gz"), None))
    return jax.shard_map(
        on_device,
        mesh=mesh,
        in_specs=placed,
        out_specs=P(("rep", "gz"), "gy", None),
        check_vma=False,
    )
```

```python
import functools
import math

import jax
import jax.numpy as jnp
import numpy as np
from jax import lax
from jax.experimental import pallas as pl
from jax.experimental.pallas import tpu as pltpu
from jax.sharding import PartitionSpec as P

NG = 256
NZ = 128


two_pi = 2.0 * math.pi
highest = lax.Precision.HIGHEST


def tables(length, rows_index, cols_index):
    phase = rows_index[:, None] * cols_index[None, :] % length
    angle = phase.astype(jnp.float32) * (two_pi / length)
    return (jnp.cos(angle), jnp.sin(angle))


def reflect(values):
    return jnp.roll(jnp.flip(values, (1, 2)), (1, 1), axis=(1, 2))


def slab_plan(charges, green):
    gy_count = lax.axis_size("gy")
    gz_count = lax.axis_size("gz")
    groups = gy_count * gz_count
    half = NZ // 2
    per_device = half // groups
    col_block = charges.shape[1]
    depth = jnp.arange(NZ, dtype=jnp.int32)
    bins = jnp.arange(half, dtype=jnp.int32)
    indices = jnp.arange(NG, dtype=jnp.int32)
    cos_depth, sin_depth = tables(NZ, depth, bins)
    alternate = (1 - 2 * (depth % 2)).astype(jnp.float32)
    sin_packed = jnp.where(bins[None, :] == 0, -alternate[:, None], sin_depth)
    spec_re = jnp.einsum("xyz,zk->kxy", charges, cos_depth, precision=highest)
    spec_im = -jnp.einsum("xyz,zk->kxy", charges, sin_packed, precision=highest)
    own = jnp.moveaxis(green[:, :, :half], 2, 0)
    mirror = jnp.concatenate(
        [green[:, :, half : half + 1], jnp.flip(green[:, :, half + 1 :], 2)], axis=2
    )
    mirror = jnp.moveaxis(mirror, 2, 0)
    own, mirror = (
        lax.all_to_all(own, ("gy", "gz"), split_axis=0, concat_axis=2, tiled=True),
        lax.all_to_all(mirror, ("gy", "gz"), split_axis=0, concat_axis=2, tiled=True),
    )
    own, mirror = (
        lax.all_gather(own, "rep", axis=1, tiled=True),
        lax.all_gather(mirror, "rep", axis=1, tiled=True),
    )
    plane_re, plane_im = (
        lax.all_to_all(spec_re, ("gy", "gz"), split_axis=0, concat_axis=1, tiled=True),
        lax.all_to_all(spec_im, ("gy", "gz"), split_axis=0, concat_axis=1, tiled=True),
    )
    plane_re = plane_re.reshape(per_device, gy_count, NG, col_block)
    plane_im = plane_im.reshape(per_device, gy_count, NG, col_block)
    cos_plain, sin_plain = tables(NG, indices, indices)
    wide_cos = cos_plain.reshape(NG, gy_count, col_block)
    wide_sin = sin_plain.reshape(NG, gy_count, col_block)

    def second_in(matrix, values):
        return jnp.einsum("kgc,bgxc->bxk", matrix, values, precision=highest)

    def first_in(matrix, values):
        return jnp.einsum("kx,bxj->bkj", matrix, values, precision=highest)

    inner_re = second_in(wide_cos, plane_re) + second_in(wide_sin, plane_im)
    inner_im = second_in(wide_cos, plane_im) - second_in(wide_sin, plane_re)
    freq_re = first_in(cos_plain, inner_re) + first_in(sin_plain, inner_im)
    freq_im = first_in(cos_plain, inner_im) - first_in(sin_plain, inner_re)
    slot = lax.axis_index("gy") * gz_count + lax.axis_index("gz")
    packed = ((slot == 0) & (jnp.arange(per_device) == 0))[:, None, None]
    plain_gain = 0.5 * (own + reflect(mirror))
    first_gain = jnp.where(packed, 0.5 * (own + reflect(own)), plain_gain)
    second_gain = jnp.where(packed, 0.5 * (mirror + reflect(mirror)), plain_gain)
    mean_gain = 0.5 * (first_gain + second_gain)
    odd_gain = 0.5 * (first_gain - second_gain)
    prod_re = freq_re * mean_gain + reflect(freq_re) * odd_gain
    prod_im = freq_im * mean_gain - reflect(freq_im) * odd_gain
    undo_re = first_in(cos_plain, prod_re) - first_in(sin_plain, prod_im)
    undo_im = first_in(sin_plain, prod_re) + first_in(cos_plain, prod_im)

    def second_out(matrix, values):
        return jnp.einsum("kgc,bxk->bgxc", matrix, values, precision=highest)

    cells_re = second_out(wide_cos, undo_re) - second_out(wide_sin, undo_im)
    cells_im = second_out(wide_sin, undo_re) + second_out(wide_cos, undo_im)
    cells_re = cells_re.reshape(per_device, gy_count * NG, col_block)
    cells_im = cells_im.reshape(per_device, gy_count * NG, col_block)
    home_re, home_im = (
        lax.all_to_all(cells_re, ("gy", "gz"), split_axis=1, concat_axis=0, tiled=True),
        lax.all_to_all(cells_im, ("gy", "gz"), split_axis=1, concat_axis=0, tiled=True),
    )
    weight = jnp.where(bins == 0, 1.0, 2.0).astype(jnp.float32)
    cos_back = (cos_depth * weight[None, :]).T
    sin_back = jnp.where(bins[:, None] == 0, alternate[None, :], -2.0 * sin_depth.T)
    result_field = jnp.einsum("kxy,kz->xyz", home_re, cos_back, precision=highest)
    result_field = result_field + jnp.einsum("kxy,kz->xyz", home_im, sin_back, precision=highest)
    return result_field / (NG * NG * NZ)


f32 = jnp.float32
bf16 = jnp.bfloat16
MESH = pl.DeviceIdType.MESH
PARTS = 2
HALVES = 2


def split(values):
    high = values.astype(bf16)
    return high, (values - high.astype(f32)).astype(bf16)


def stacked_table(table, axis):
    rounded = table.astype(jnp.bfloat16)
    return jnp.asarray(np.stack([rounded, (table - rounded.astype(np.float64)).astype(jnp.bfloat16)], axis=axis))


def dot(left, right, dims=((1,), (0,))):
    return lax.dot_general(left, right, (dims, ((), ())), preferred_element_type=f32)


def dot_table(values, table_high, table_low, dims=((1,), (0,))):
    high, low = split(values)
    return dot(high, table_high, dims) + (dot(low, table_high, dims) + dot(high, table_low, dims))


def table_dot(table_high, table_low, values, dims=((1,), (0,))):
    high, low = split(values)
    return dot(table_high, high, dims) + (dot(table_high, low, dims) + dot(table_low, high, dims))


def depth_tables(length, groups, bins_each):
    per_part = bins_each // PARTS
    forward, back = [], []
    z = np.arange(length)
    alternate = 1.0 - 2.0 * (z % 2)
    for start in range(0, groups * bins_each, per_part):
        for imaginary in (False, True):
            for k in range(start, start + per_part):
                angle = 2.0 * np.pi * ((k * z) % length) / length
                if k == 0:
                    forward.append(alternate if imaginary else np.ones(length))
                    back.append(alternate if imaginary else np.ones(length))
                else:
                    forward.append(-np.sin(angle) if imaginary else np.cos(angle))
                    back.append(-2.0 * np.sin(angle) if imaginary else 2.0 * np.cos(angle))
    return np.stack(forward), np.stack(back)


def wide_table(table, axis):
    rounded = table.astype(jnp.bfloat16)
    low = (table - rounded.astype(np.float64)).astype(jnp.bfloat16)
    both = np.concatenate([rounded, rounded], axis=1 - axis)
    return jnp.asarray(np.concatenate([both, np.concatenate([low, np.zeros_like(low)], axis=1 - axis)], axis=axis))


def depth_in(table, cells, out):
    groups, parts, _, cols = out.shape
    rows, depth, step = cells.shape[0], cells.shape[2], 8

    def body(i, carry):
        values = jnp.concatenate(split(cells[pl.ds(i * step, step)].reshape(step * cols, depth)), axis=1)
        both = dot(table[...], values, ((1,), (1,)))
        result = both[:depth] + both[depth:]
        for row in range(step):
            piece = result[:, row * cols : (row + 1) * cols]
            at = pl.multiple_of(i * (step * 8) + row * 8, 8)
            out[:, :, pl.ds(at, 8), :] = piece.reshape(groups, parts, 8, cols)
        return carry

    lax.fori_loop(0, rows // step, body, 0)


def depth_out_kernel(table_ref, spec_ref, out_ref, held, sem):
    rows, cols, depth = out_ref.shape
    step = rows // sem.shape[0]
    copies = []
    for start in range(0, rows, step):
        pieces = [spec_ref[:, :, row * 8 : (row + 1) * 8, :].reshape(depth, cols) for row in range(start, start + step)]
        values = jnp.concatenate(split(jnp.concatenate(pieces, axis=1)), axis=0)
        both = dot(values, table_ref[...], ((0,), (0,)))
        at = pl.ds(start, step)
        held[at] = (both[:, :depth] + both[:, depth:]).reshape(step, cols, depth)
        copies.append(pltpu.make_async_copy(held.at[at], out_ref.at[at], sem.at[start // step]))
        copies[-1].start()
    for copy in copies:
        copy.wait()


def green_terms(count, green_ref):
    size, pitch, lanes = green_ref.shape
    flat = green_ref.reshape(size * pitch, lanes)
    rest = jnp.concatenate([flat[pl.ds(k2, size, stride=pitch), :] for k2 in range(count)], axis=0)
    return jnp.concatenate(split(rest), axis=1)


def pick_green(part, pick_ref, terms, out_ref):
    groups, parts, halves, rows, _ = out_ref.shape
    size = groups * halves * 8
    pick = pick_ref[part * 2 * size : (part + 1) * 2 * size, :]
    result = dot(jnp.concatenate([pick, pick], axis=1), terms, ((1,), (1,)))
    first_lanes = lax.broadcasted_iota(jnp.int32, (size, 128), 1) < 64
    place = lax.rem(lax.broadcasted_iota(jnp.int32, (size, 128), 0), 8) // 2
    even = (place == 0) | (place == 2)
    stays = first_lanes == even
    for tile in range(rows // 8):
        own, mirror = (
            jnp.where(
                place < 2, result[start : start + size, tile * 256 : tile * 256 + 128],
                result[start : start + size, tile * 256 + 128 : (tile + 1) * 256])
            for start in (0, size)
        )
        packed = jnp.where(
            stays, jnp.where(even, own, mirror), pltpu.roll(jnp.where(even, mirror, own), 64, 1))
        out_ref[:, part, :, tile * 8 : (tile + 1) * 8, :] = packed.reshape(groups, halves, 8, 128)


def planes_kernel(
    gy_count, gz_count, reps,
    cells_in, green_in, pick_in, depth_table, waves_ref, flips_ref, home_ref,
    cells_ref, field_ref, pick_ref, depth_ref, gains_ref, spec_ref,
    planes, green, freq, waves, tables, flips,
    fwd_send, fwd_recv, back_send, back_recv, green_send, green_recv, right_send, left_send, line_recv, own_sem, table_sem, in_sem,
):
    groups = gy_count * gz_count
    rep, gy, gz = lax.axis_index("rep"), lax.axis_index("gy"), lax.axis_index("gz")
    slot = gy * gz_count + gz
    rows = spec_ref.shape[2] // 8
    ng = flips_ref.shape[0]
    piece = gains_ref.shape[3]
    quarters = [(part, half) for part in range(PARTS) for half in range(HALVES)]

    def partner(step):
        there_y = lax.rem(gy + step // gz_count, gy_count)
        there_z = lax.rem(gz + step % gz_count, gz_count)
        return there_y * gz_count + there_z, {"rep": rep, "gy": there_y, "gz": there_z}

    def along(step):
        return {"rep": lax.rem(rep + step + reps, reps), "gy": gy, "gz": gz}

    inputs = [
        pltpu.make_async_copy(source, held, in_sem.at[i])
        for i, (source, held) in enumerate((
            (green_in, field_ref.at[:, pl.ds(0, green_in.shape[1]), :]), (pick_in, pick_ref), (cells_in, cells_ref), (depth_table, depth_ref)))
    ]

    loads = [
        pltpu.make_async_copy(source, held, table_sem.at[i])
        for i, (source, held) in enumerate(((waves_ref, waves), (flips_ref, flips)))
    ]

    order = sorted(
        range(1, groups), key=lambda s: (s % gz_count == 0, s < gz_count, abs(s % gz_count - gz_count // 2), -s))

    barrier = pltpu.get_barrier_semaphore()
    for step in order:
        pl.semaphore_signal(barrier, inc=1, device_id=partner(step)[1], device_id_type=MESH)

    @pl.when(rep + 1 < reps)
    def _():
        pl.semaphore_signal(barrier, inc=1, device_id=along(1), device_id_type=MESH)

    @pl.when(rep >= 1)
    def _():
        pl.semaphore_signal(barrier, inc=1, device_id=along(-1), device_id_type=MESH)

    for copy in inputs[:2]:
        copy.start()
    for copy in inputs[:2]:
        copy.wait()
    for copy in inputs[2:]:
        copy.start()
    terms = green_terms(green_in.shape[1], field_ref)
    pick_green(0, pick_ref, terms, gains_ref)
    pl.semaphore_wait(barrier, groups - 1 + lax.div(rep + reps - 1, reps) + lax.div(2 * reps - 2 - rep, reps))

    def green_copy(step, source, part, half):
        there, device = partner(step)
        return pltpu.make_async_remote_copy(
            src_ref=gains_ref.at[there, part, half], dst_ref=green.at[rep, part, half, pl.ds(source * piece, piece), :],
            send_sem=green_send.at[0], recv_sem=green_recv.at[part, half],
            device_id=device, device_id_type=MESH)

    def fwd_copy(step, source, part):
        there, device = partner(step)
        return pltpu.make_async_remote_copy(
            src_ref=spec_ref.at[there, part], dst_ref=planes.at[source, part],
            send_sem=fwd_send.at[0], recv_sem=fwd_recv.at[part], device_id=device, device_id_type=MESH)

    def back_copy(step, source, part):
        there, device = partner(step)
        return pltpu.make_async_remote_copy(
            src_ref=planes.at[there, part], dst_ref=home_ref.at[source, part],
            send_sem=back_send.at[0], recv_sem=back_recv.at[0], device_id=device, device_id_type=MESH)

    def whole(ref, sem):
        return pltpu.make_async_remote_copy(
            src_ref=ref, dst_ref=ref, send_sem=sem, recv_sem=sem, device_id=partner(1)[1], device_id_type=MESH)

    def line_copy(block, at, sem, step):
        return pltpu.make_async_remote_copy(
            src_ref=green.at[(block, *at)], dst_ref=green.at[(block, *at)], send_sem=sem,
            recv_sem=line_recv.at[(block, *at)], device_id=along(step), device_id_type=MESH)

    def green_start(part):
        for half in range(HALVES):
            for step in order:
                green_copy(step, slot, part, half).start()

    green_start(0)
    for part in range(1, PARTS):
        pick_green(part, pick_ref, terms, gains_ref)
        green_start(part)
    for part, half in quarters:
        green[rep, part, half, pl.ds(slot * piece, piece), :] = gains_ref[slot, part, half]
    for copy in inputs[2:]:
        copy.wait()
    for load in loads:
        load.start()
    depth_in(depth_ref, cells_ref, spec_ref)
    for part in range(PARTS):
        for step in order:
            fwd_copy(step, slot, part).start()
    planes[slot] = spec_ref[slot]
    others = pl.ds(0, groups - 1)

    def green_wait(at):
        whole(green.at[(rep, *at, pl.ds(0, (groups - 1) * piece))], green_recv.at[at]).wait_recv()

    def line_start(at, hop=None):
        right, left = rep + 1 < reps, rep >= 1
        if hop is not None:
            right, left = right & (rep == hop), left & (rep + hop == reps - 1)

        @pl.when(right)
        def _():
            line_copy(rep, at, right_send.at[0], 1).start()

        @pl.when(left)
        def _():
            line_copy(rep, at, left_send.at[0], -1).start()

    def relay(hop, at):
        @pl.when((rep >= hop) & (rep + 1 < reps))
        def _():
            line_copy(rep - hop, at, right_send.at[0], 1).wait_recv()
            line_copy(rep - hop, at, right_send.at[0], 1).start()

        @pl.when((rep + hop < reps) & (rep >= 1))
        def _():
            line_copy(rep + hop, at, left_send.at[0], -1).wait_recv()
            line_copy(rep + hop, at, left_send.at[0], -1).start()

    def line_end(at):
        for hop in range(1, reps):
            @pl.when(rep + 1 == reps)
            def _():
                line_copy(rep - hop, at, right_send.at[0], 1).wait_recv()

            @pl.when(rep == 0)
            def _():
                line_copy(rep + hop, at, left_send.at[0], -1).wait_recv()

    def load_plane(part, row):
        bands = []
        for y in range(gy_count):
            bands.append(jnp.concatenate(
                [planes[y * gz_count + x, part, pl.ds(row, rows, stride=8), :] for x in range(gz_count)], axis=0))
        return jnp.concatenate(bands, axis=1)

    def forward(part):
        def body(p, carry):
            values = jnp.concatenate([load_plane(part, p), load_plane(part, 4 + p)], axis=1)
            inner = dot_table(values, tables[0, 0], tables[0, 1])
            inner = jnp.concatenate([inner[:, :ng], inner[:, ng:]], axis=0)
            freq[part * 4 + p] = table_dot(tables[1, 0], tables[1, 1], inner)
            return carry

        lax.fori_loop(0, 4, body, 0)

    def reflect_plane(values):
        high, low = split(values)
        turned = dot(flips[...], high) + dot(flips[...], low)
        high, low = split(turned)
        return dot(high, flips[...]) + dot(low, flips[...])

    def backward(part, half):
        def body(p):
            row = half * 2 + p
            plane = part * 4 + row
            own, mirror = [], []
            lane = lax.broadcasted_iota(jnp.int32, (ng, 128), 1)
            for r in range(0, reps, 2):
                one, two = (green[q, part, half, pl.ds(p, ng, stride=2), :] for q in (r, r + 1))
                own.append(jnp.where(lane < 64, one, pltpu.roll(two, 64, 1)))
                mirror.append(jnp.where(lane < 64, pltpu.roll(one, 64, 1), two))
            own = jnp.concatenate(own, axis=1).T
            mirror = jnp.concatenate(mirror, axis=1).T

            def plain():
                gain = 0.5 * (own + reflect_plane(mirror))
                freq[plane] = freq[plane] * jnp.concatenate([gain, gain], axis=0)

            if plane == 0:
                packed = slot == 0

                @pl.when(jnp.logical_not(packed))
                def _():
                    plain()

                @pl.when(packed)
                def _():
                    first = 0.5 * (own + reflect_plane(own))
                    second = 0.5 * (mirror + reflect_plane(mirror))
                    mean, odd = 0.5 * (first + second), 0.5 * (first - second)
                    real, imag = freq[plane, :ng, :], freq[plane, ng:, :]
                    freq[plane, :ng, :] = real * mean + reflect_plane(real) * odd
                    freq[plane, ng:, :] = imag * mean - reflect_plane(imag) * odd
            else:
                plain()

            undo = table_dot(tables[0, 0], tables[0, 1], freq[plane])
            undo = jnp.concatenate([undo[:ng], undo[ng:]], axis=1)
            cells = dot_table(undo, tables[1, 0], tables[1, 1])
            cols = ng // gy_count
            for c in range(2):
                for y in range(gy_count):
                    for x in range(gz_count):
                        planes[y * gz_count + x, part, pl.ds(c * 4 + row, rows, stride=8), :] = cells[
                            x * rows : (x + 1) * rows, c * ng + y * cols : c * ng + (y + 1) * cols]

        for p in range(2):
            body(p)

    own_home = [pltpu.make_async_copy(planes.at[slot, h], home_ref.at[slot, h], own_sem.at[0]) for h in range(PARTS)]

    def arrive(part):
        whole(planes.at[others, part], fwd_recv.at[part]).wait_recv()
        forward(part)

    def depart(part):
        for step in order:
            back_copy(step, slot, part).start()
        own_home[part].start()

    first, second = quarters[:HALVES], quarters[HALVES:]

    def second_relay(hop):
        relay(hop, second[0])
        line_start(second[1], hop)

    for at in first:
        green_wait(at)
        line_start(at)
    relay(1, first[0])
    for at in second:
        green_wait(at)
    for at in second:
        line_start(at, 0)
    relay(1, first[1])
    line_start(second[0], 1)
    for hop in range(2, reps - 1):
        for at in first:
            relay(hop, at)
        line_start(second[0], hop)
    for load in loads:
        load.wait()
    for table, swap in enumerate((False, True)):
        minus, plus = (1, 2) if swap else (2, 1)
        for quadrant, wave in enumerate((0, minus, plus, 0)):
            down, right = quadrant // 2 * ng, quadrant % 2 * ng
            tables[table, :, down : down + ng, right : right + ng] = waves[wave]
    second_relay(1)
    arrive(0)
    for at in first:
        line_end(at)
        backward(*at)
        if at == first[0]:
            for hop in range(2, reps - 1):
                second_relay(hop)
    depart(0)
    for hop in range(1, reps - 1):
        relay(hop, second[1])
    arrive(1)
    for at in second:
        line_end(at)
        backward(*at)
    depart(1)

    whole(gains_ref.at[others], green_send.at[0]).wait_send()
    whole(spec_ref.at[others], fwd_send.at[0]).wait_send()
    for at in range(1, reps):
        @pl.when(rep + 1 == at)
        def _():
            whole(green.at[pl.ds(0, at)], right_send.at[0]).wait_send()

        @pl.when(rep == at)
        def _():
            whole(green.at[pl.ds(at, reps - at)], left_send.at[0]).wait_send()
    pltpu.make_async_copy(planes.at[slot], home_ref.at[slot], own_sem.at[0]).wait()
    whole(planes.at[others], back_send.at[0]).wait_send()
    whole(home_ref.at[others], back_recv.at[0]).wait_recv()


def fused_plan(charges, green):
    gy_count, gz_count, reps = lax.axis_size("gy"), lax.axis_size("gz"), lax.axis_size("rep")
    groups = gy_count * gz_count
    rows, cols, depth = charges.shape
    ng = rows * gz_count
    half = depth // 2
    each = half // groups
    forward_table, back_table = depth_tables(depth, groups, each)
    chunks = rows // 8
    spec_shape = jax.ShapeDtypeStruct((groups, PARTS, rows * 8, cols), f32)

    k1, k2, _ = green.shape
    own_index = np.arange(half)
    opposite = np.where(own_index == 0, half, depth - own_index)
    quad, place = np.divmod(np.arange(groups * HALVES * 8), 8)
    quad = quad // HALVES * PARTS * HALVES + quad % HALVES
    pick = []
    for part in range(PARTS):
        bins = (quad + part * HALVES) * 2 + place % 2
        pick += [own_index[bins], opposite[bins]]
    pick = (np.concatenate(pick)[:, None] == np.arange(depth)[None, :]).astype(np.float32)
    index = np.arange(ng)
    angle = 2.0 * np.pi * ((index[:, None] * index[None, :]) % ng) / ng
    cos, sin = np.cos(angle), np.sin(angle)
    waves = stacked_table(np.stack([cos, sin, -sin]), 1)
    flips = jnp.asarray((index[:, None] + index[None, :]) % ng == 0, bf16)

    dma = pltpu.SemaphoreType.DMA
    home = pl.pallas_call(
        functools.partial(planes_kernel, gy_count, gz_count, reps),
        out_shape=spec_shape, name="planes",
        in_specs=[pl.BlockSpec(memory_space=pl.ANY)] * 6, out_specs=pl.BlockSpec(memory_space=pl.ANY),
        scratch_shapes=[
            pltpu.VMEM(charges.shape, f32),
            pltpu.VMEM((k1, k2 + 8, depth), f32),
            pltpu.VMEM(pick.shape, bf16),
            pltpu.VMEM((2 * depth, 2 * depth), bf16),
            pltpu.VMEM((groups, PARTS, HALVES, k2 * 2, 2 * k1), f32),
            pltpu.VMEM(spec_shape.shape, f32),
            pltpu.VMEM(spec_shape.shape, f32),
            pltpu.VMEM((reps, PARTS, HALVES, ng * 2, 2 * k1), f32),
            pltpu.VMEM((each, 2 * ng, ng), f32),
            pltpu.VMEM(waves.shape, bf16),
            pltpu.VMEM((2, 2, 2 * ng, 2 * ng), bf16),
            pltpu.VMEM((ng, ng), bf16),
            dma((1,)), dma((PARTS,)), dma((1,)), dma((1,)), dma((1,)), dma((PARTS, HALVES)),
            dma((1,)), dma((1,)), dma((reps, PARTS, HALVES)), dma((1,)), dma((2,)), dma((4,)),
        ],
        compiler_params=pltpu.CompilerParams(
            collective_id=0, has_side_effects=True, vmem_limit_bytes=44 * 2**20),
    )(*(
        pltpu.with_memory_space_constraint(value, pltpu.HBM)
        for value in (
            charges, green, jnp.asarray(pick, bf16), wide_table(forward_table, 0), waves, flips)
    ))

    vmem = pl.BlockSpec(memory_space=pltpu.VMEM)
    return pl.pallas_call(
        depth_out_kernel, out_shape=jax.ShapeDtypeStruct(charges.shape, f32), name="depth_out",
        in_specs=[vmem, vmem], out_specs=pl.BlockSpec(memory_space=pl.ANY),
        scratch_shapes=[pltpu.VMEM(charges.shape, f32), dma((chunks,))],
        compiler_params=pltpu.CompilerParams(vmem_limit_bytes=16 * 2**20),
    )(wide_table(back_table / (ng * ng * depth), 1), home)


def on_device(charges, green):
    groups = lax.axis_size("gy") * lax.axis_size("gz")
    rows, cols, depth = charges.shape
    aligned = (
        cols % 128 == 0 and depth % 128 == 0 and depth == 16 * groups and rows % 8 == 0
        and green.shape[0] == 64 and lax.axis_size("rep") % 2 == 0 and lax.axis_size("rep") > 2
        and rows * lax.axis_size("gz") == cols * lax.axis_size("gy")
    )
    return fused_plan(charges, green) if aligned else slab_plan(charges, green)


def solution(mesh):
    placed = (P(("rep", "gz"), "gy", None), P("rep", ("gy", "gz"), None))
    return jax.shard_map(
        on_device,
        mesh=mesh,
        in_specs=placed,
        out_specs=P(("rep", "gz"), "gy", None),
        check_vma=False,
    )
```
